128 devices in a mesh: genes: 64 (over z, y, x_hi, core), cols: 2 (over x_lo).
Axes of the slice: x: 4 (x_hi: 2, x_lo: 2; x = x_hi * 2 + x_lo), y: 4, z: 4, core: 2. Of those that a mesh axis runs over, the one named last changes fastest.
Arguments:
- expression: float32 [384, 40960], P(None, ('genes', 'cols')), may hold values from -200 to 200
- resample: int32 [384], replicated, may hold values from 0 to 383
- labels: int32 [40960, 300], P(('genes', 'cols')), may hold values from 0 to 1, as said below
- ref_kim: float32 [40960], P(('genes', 'cols')), may hold values from 0 to 1
Outputs:
- connectivity: float32 [40960, 300], P(('genes', 'cols'))
- preservation: float32 [2, 300], replicated
The draws below stay inside these ranges and needn't reach their ends.
Inputs may be any that keep to these rules, and one draw needn't show every extreme that they name: `labels`: each row holds exactly one 1; every module has 32 or more genes.
All inputs are finite; a program needn't handle non-finite values.
Results may differ from the reference program's by a relative error of at most 0.0031.
Values may be sent and summed in bfloat16 or wider, within the bound.
A program may use at most 64 MiB of HBM per device.

```python
import math
import jax
import jax.numpy as jnp
from jax import lax

G = 40960
K = 300
SAMPLES = 384
MIN_MODULE = 32


def gene_modules(key):
    order = jax.random.permutation(jax.random.fold_in(key, 11), G)
    position = jnp.arange(G, dtype=jnp.int32)
    extra = jax.random.randint(jax.random.fold_in(key, 12), (G,), 0, K, dtype=jnp.int32)
    at_position = jnp.where(position < K * MIN_MODULE, position % K, extra)
    return jnp.zeros((G,), jnp.int32).at[order].set(at_position)


def draw_labels(key, part):
    module_ids = gene_modules(key)
    return (module_ids[:, None] == jnp.arange(K, dtype=jnp.int32)[None, :]).astype(jnp.int32)


def shared_signal(key, module_ids):
    meta_count = 8
    meta = jnp.clip(jax.random.normal(jax.random.fold_in(key, 26), (SAMPLES, meta_count), jnp.float32), -6.0, 6.0)
    mixing = jax.random.uniform(jax.random.fold_in(key, 27), (meta_count, K), jnp.float32, 0.3, 1.0)
    mixing = mixing / jnp.sqrt(jnp.sum(mixing * mixing, axis=0, keepdims=True))
    shares = jax.random.uniform(jax.random.fold_in(key, 28), (K,), jnp.float32, 0.4, 0.8)
    own = jnp.clip(jax.random.normal(jax.random.fold_in(key, 21), (SAMPLES, K), jnp.float32), -6.0, 6.0)
    common = jnp.dot(meta, mixing, precision=lax.Precision.HIGHEST, preferred_element_type=jnp.float32)
    factor = jnp.clip(jnp.sqrt(shares)[None, :] * common + jnp.sqrt(1.0 - shares)[None, :] * own, -6.0, 6.0)
    loading = jax.random.uniform(jax.random.fold_in(key, 22), (G,), jnp.float32, 0.5, 2.0)
    gene_mix = jax.random.normal(jax.random.fold_in(key, 29), (meta_count, G), jnp.float32) / jnp.sqrt(jnp.float32(meta_count))
    direct = jnp.clip(0.4 * jnp.dot(meta, gene_mix, precision=lax.Precision.HIGHEST, preferred_element_type=jnp.float32), -3.0, 3.0)
    return jnp.take(factor, module_ids, axis=1) * loading[None, :] + direct


def draw_expression(key, part):
    module_ids = gene_modules(key)
    signal = shared_signal(key, module_ids)
    noise = jnp.clip(jax.random.normal(jax.random.fold_in(key, 23), (SAMPLES, G), jnp.float32), -6.0, 6.0)
    return signal + noise


def place_ends(array, key, least, top_value):
    shape = array.shape
    spot = [jax.random.randint(jax.random.fold_in(key, axis), (), 0, shape[axis]) for axis in range(len(shape))]
    array = array.at[tuple(spot)].set(least)
    longest = shape.index(max(shape))
    spot[longest] = (spot[longest] + 1) % shape[longest]
    return array.at[tuple(spot)].set(top_value)


def level_of(own_key, shape, split, least, high):
    level = 1.0
    for dim, shards_of in split:
        draws = jax.random.uniform(jax.random.fold_in(jax.random.fold_in(own_key, 6), dim), (shards_of,), jnp.float32, least / len(split), high / len(split))
        level = level * jnp.repeat(jnp.exp(draws), shape[dim] // shards_of).reshape((-1,) + (1,) * (len(shape) - 1 - dim))
    return level


def setup_inputs(seed: int = 0) -> dict:
    key_of = jax.random.split(jax.random.key(seed), 5)
    return {
        "expression": draw_expression(jax.random.fold_in(key_of[4], 71), 0),
        "resample": place_ends(jax.random.randint(key_of[1], (SAMPLES,), 0, SAMPLES), jax.random.fold_in(key_of[1], 1), 0, SAMPLES - 1).astype(jnp.int32),
        "labels": draw_labels(jax.random.fold_in(key_of[4], 71), 0),
        "ref_kim": jnp.clip(1.0 * jax.random.uniform(key_of[3], (G,), jnp.float32) ** level_of(key_of[3], (G,), ((0, 128),), -0.2, 0.2), 0.0, 1.0),
    }


def standardize(expression, resample):
    boot = jnp.take(expression, resample, axis=0)
    centered = boot - lax.optimization_barrier(jnp.mean(boot, axis=0, keepdims=True))
    total = lax.optimization_barrier(jnp.sum(centered * centered, axis=0, keepdims=True))
    return (centered * lax.rsqrt(total + 1e-06)).astype(jnp.bfloat16)

def local_sums(connectivity, labels, ref_kim):
    member = labels.astype(jnp.float32)
    kim = lax.optimization_barrier(jnp.sum(connectivity * member, axis=1))
    rowsum = lax.optimization_barrier(jnp.sum(connectivity, axis=1))
    stacked = jnp.stack([kim, kim * kim, ref_kim, ref_kim * ref_kim, kim * ref_kim, rowsum, jnp.ones_like(kim)], axis=1)
    return jnp.dot(member.T, stacked, precision=lax.Precision.HIGHEST, preferred_element_type=jnp.float32)

def preserve(sums, total_genes):
    counts = sums[:, 6]
    mean_x = sums[:, 0] / (counts * counts)
    var_x = jnp.maximum(sums[:, 1] / (counts * counts * counts) - mean_x * mean_x, 0.0001)
    mean_y = sums[:, 2] / counts
    var_y = jnp.maximum(sums[:, 3] / counts - mean_y * mean_y, 0.01)
    cross = sums[:, 4] / (counts * counts) - mean_x * mean_y
    between = (sums[:, 5] - sums[:, 0]) / (counts * (total_genes - counts))
    density = (mean_x - between) * jnp.sqrt(counts / var_x)
    linked = cross * jnp.sqrt(counts / (var_x * var_y))
    return jnp.stack([density, linked], axis=0)

def reference(expression, resample, labels, ref_kim):
    scaled = standardize(expression, resample)
    member_bf = labels.astype(jnp.bfloat16)
    block_rows = math.gcd(G, 512)

    def one_block(block_index):
        rows = lax.dynamic_slice_in_dim(scaled, block_index * block_rows, block_rows, 1)
        scores = lax.dot_general(rows, scaled, (((0,), (0,)), ((), ())), preferred_element_type=jnp.float32)
        squares = scores * scores
        adjacency = (squares * squares * squares).astype(jnp.bfloat16)
        return jnp.dot(adjacency, member_bf, preferred_element_type=jnp.float32)
    pieces = lax.map(one_block, jnp.arange(G // block_rows, dtype=jnp.int32))
    connectivity = pieces.reshape(G, K)
    sums = local_sums(connectivity, labels, ref_kim)
    return (connectivity, preserve(sums, G))
```

```python
import functools

import jax
import jax.numpy as jnp
from jax import lax
from jax.experimental import pallas as pl
from jax.experimental.pallas import tpu as pltpu
from jax.sharding import Mesh
from jax.sharding import PartitionSpec as P

G = 40960
SAMPLES = 384
K = 300
KP = 304
OWN = 320
HALF = OWN // 2
LINE = 4
CHUNK = 2 * OWN
STEP = 2 * LINE * HALF
ROWS = LINE * CHUNK
COLS = LINE * STEP
TILE = 512
TILES = ROWS // TILE
KEEP = 384
AXES = ("z", "y", "xh", "c", "xl")
OFFSETS = (0, 1, 3, 2)
SEEN_AS = (0, 2, 1, 3)
NT = (((1,), (1,)), ((), ()))


def kernel(
    depth, compact, resample, expression, labels, ref_kim, conn_out, pres_out,
    rows, cols, lt, adj, acc, pair, sent, got, own_ids, member, sums_xc, sums_y, sums_z,
    send_rows, recv_rows, send_fwd, recv_fwd, send_near, recv_near, send_far, recv_far,
    send_pair, recv_pair, send_sum, recv_sum, send_xc, recv_xc, send_yz, recv_yz,
):
    f32, bf16 = jnp.float32, jnp.bfloat16
    z, y, core = lax.axis_index("z"), lax.axis_index("y"), lax.axis_index("c")
    x = lax.axis_index("xh") * 2 + lax.axis_index("xl")
    other = 1 - core

    def at_x(place, c=None):
        there = lax.rem(x + OFFSETS[place], LINE)
        device = {"xh": there // 2, "xl": lax.rem(there, 2)}
        if c is not None:
            device["c"] = c
        return device

    def at_y(place):
        return {"y": lax.rem(y + OFFSETS[place], LINE)}

    def at_z(place):
        return {"z": lax.rem(z + OFFSETS[place], LINE)}

    partner = {"c": other}

    barrier = pltpu.get_barrier_semaphore()
    peers = [partner]
    for place in range(1, LINE):
        peers += [at_x(place), at_x(place, other), at_y(place), at_z(place)]
    for peer in peers:
        pl.semaphore_signal(barrier, inc=1, device_id=peer, device_id_type=pl.DeviceIdType.MESH)

    def remote(src, dst, send_sem, recv_sem, device):
        return pltpu.make_async_remote_copy(
            src_ref=src, dst_ref=dst, send_sem=send_sem, recv_sem=recv_sem,
            device_id=device, device_id_type=pl.DeviceIdType.MESH,
        )

    started = []

    def send(*args):
        copy = remote(*args)
        copy.start()
        started.append(copy)

    drawn = resample[...]
    ones_at = lax.broadcasted_iota(jnp.int32, (SAMPLES, SAMPLES), 0) == drawn
    hits = jnp.where(ones_at, 1.0, 0.0)
    times = jnp.sum(hits, axis=1, keepdims=True)
    if compact:
        times_row = lax.dot_general(
            jnp.ones((16, SAMPLES), bf16), hits.astype(bf16), NT, preferred_element_type=f32
        )
        present = jnp.where(times_row > 0.5, 1.0, 0.0)
        before = jnp.where(
            lax.broadcasted_iota(jnp.int32, (SAMPLES, SAMPLES), 0)
            < lax.broadcasted_iota(jnp.int32, (SAMPLES, SAMPLES), 1),
            1.0,
            0.0,
        ).astype(bf16)
        rank = jnp.dot(present.astype(bf16), before, preferred_element_type=f32)
        rank = jnp.where(present > 0.5, rank, -1.0)[0:1, :]
        place_of = rank.astype(jnp.int32)
    else:
        place_of = lax.broadcasted_iota(jnp.int32, (1, SAMPLES), 1)
    pick = jnp.where(
        lax.broadcasted_iota(jnp.int32, (depth, SAMPLES), 0) == place_of, 1.0, 0.0
    ).astype(bf16)
    values = expression[...]
    mean = jnp.sum(values * times, axis=0, keepdims=True) * (1.0 / SAMPLES)
    centered = values - mean
    total = jnp.sum(centered * centered * times, axis=0, keepdims=True)
    scaled = (centered * lax.rsqrt(total + 1e-06)).astype(bf16)
    weighted = (scaled.astype(f32) * times).astype(bf16)
    over_samples = (((0,), (1,)), ((), ()))
    side = lax.dot_general(weighted, pick, over_samples, preferred_element_type=f32)
    front = lax.dot_general(scaled, pick, over_samples, preferred_element_type=f32)
    marks = labels[...].astype(f32)
    module = lax.broadcasted_iota(jnp.int32, (OWN, K), 1).astype(f32) - 150.0
    id_column = jnp.sum(marks * module, axis=1, keepdims=True)
    lane = lax.broadcasted_iota(jnp.int32, (OWN, depth), 1)
    front = jnp.where(lane == depth - 1, id_column, front).astype(bf16)
    rows[pl.ds(pl.multiple_of(core * OWN, OWN), OWN), :] = side.astype(bf16)
    cols[0:HALF, :] = front[0:HALF]
    cols[STEP // 2 : STEP // 2 + HALF, :] = front[HALF:OWN]

    pl.semaphore_wait(barrier, len(peers))

    def row_block(chunk, c):
        return rows.at[pl.ds(pl.multiple_of(chunk * CHUNK + c * OWN, OWN), OWN), :]

    def col_block(step, part, slot):
        return cols.at[pl.ds(step * STEP + part * (STEP // 2) + slot * HALF, HALF), :]

    def near_index(part, place):
        return part * LINE + place

    def far_index(part, step, slot):
        return (part * LINE + step) * LINE + slot

    along = (at_z, at_y)
    across = (at_y, at_z)
    for place in range(1, LINE):
        for part in range(2):
            send(
                col_block(0, part, 0), col_block(0, part, SEEN_AS[place]),
                send_near.at[near_index(part, place)],
                recv_near.at[near_index(part, SEEN_AS[place])], along[part](place),
            )
        send(
            row_block(0, core), row_block(SEEN_AS[place], core),
            send_rows.at[place], recv_rows.at[SEEN_AS[place]], at_x(place),
        )
        if place == 1:
            send(row_block(0, core), row_block(0, core), send_fwd.at[0], recv_fwd.at[0], partner)

    def forward_columns(part, slot):
        for place in range(1, LINE):
            send(
                col_block(0, part, slot), col_block(SEEN_AS[place], part, slot),
                send_far.at[far_index(part, place, slot)],
                recv_far.at[far_index(part, SEEN_AS[place], slot)], across[part](place),
            )

    def wait_near(part, place):
        block = col_block(0, part, place)
        remote(
            block, block, send_near.at[near_index(part, place)],
            recv_near.at[near_index(part, place)], along[part](place),
        ).wait_recv()

    def wait_far(step):
        for part in range(2):
            for slot in range(LINE):
                block = col_block(step, part, slot)
                remote(
                    block, block, send_far.at[far_index(part, step, slot)],
                    recv_far.at[far_index(part, step, slot)], across[part](step),
                ).wait_recv()

    def pass_rows(chunk):
        block = row_block(chunk, core)
        remote(block, block, send_rows.at[chunk], recv_rows.at[chunk], at_x(chunk)).wait_recv()
        copy = remote(block, block, send_fwd.at[chunk], recv_fwd.at[chunk], partner)
        copy.start()

    def wait_rows(chunk):
        block = row_block(chunk, other)
        remote(block, block, send_fwd.at[chunk], recv_fwd.at[chunk], partner).wait_recv()

    for part in range(2):
        forward_columns(part, 0)

    acc[...] = jnp.zeros_like(acc)
    reach = lax.broadcasted_iota(jnp.int32, (16, K), 1).astype(f32) - 150.0
    own_ids[:, 0:OWN] = lax.dot_general(
        reach.astype(bf16), marks.astype(bf16), NT, preferred_element_type=f32
    )
    member[...] = jnp.where(
        lax.broadcasted_iota(jnp.int32, (OWN, KEEP), 1).astype(f32) - 150.0 == id_column, 1.0, 0.0
    )

    for place in range(1, LINE):
        for part in range(2):
            wait_near(part, place)
            forward_columns(part, place)
        if place < 3:
            pass_rows(place)
    wait_rows(0)

    def pair_slice(chunk, c):
        return acc.at[:, pl.ds(pl.multiple_of(chunk * CHUNK + c * 256, 128), KEEP)]

    def to_partner(chunk):
        return remote(
            pair_slice(chunk, other), pair.at[chunk], send_pair.at[chunk], recv_pair.at[chunk],
            partner,
        )

    def to_owner(chunk):
        return remote(
            sent.at[chunk], got.at[SEEN_AS[chunk]], send_sum.at[chunk],
            recv_sum.at[SEEN_AS[chunk]], at_x(chunk),
        )

    def pass_sum(chunk):
        to_partner(chunk).wait_recv()
        mine = acc[:, pl.ds(pl.multiple_of(chunk * CHUNK + core * 256, 128), KEEP)]
        sent[chunk] = (mine + pair[chunk]).astype(bf16)
        to_owner(chunk).start()

    def one_tile(t, carry):
        step, turn = t // TILES, lax.rem(t, TILES)
        tile = jnp.where(step == LINE - 1, TILES - 1 - turn, turn)
        base = pl.multiple_of(step * STEP, STEP)
        side_at = pl.multiple_of(tile * TILE, TILE)

        @pl.when(t == 1)
        def _():
            wait_rows(1)

        @pl.when(t == 2)
        def _():
            pass_rows(3)
            wait_rows(2)

        @pl.when(t == 3)
        def _():
            wait_rows(3)

        for far in range(1, LINE):

            @pl.when(t == far * TILES)
            def _():
                wait_far(far)

        @pl.when(turn == 0)
        def _():
            last = lax.broadcasted_iota(jnp.int32, (16, depth), 1) == depth - 1
            ids = lax.dot_general(
                jnp.where(last, 1.0, 0.0).astype(bf16), cols[pl.ds(base, STEP), :], NT,
                preferred_element_type=f32,
            )
            which = lax.broadcasted_iota(jnp.int32, (KP, STEP), 0).astype(f32) - 150.0
            lt[...] = jnp.where(which == ids[0:1, :], 1.0, 0.0).astype(bf16)

        side_block = rows[pl.ds(side_at, TILE), :]
        for part in range(STEP // 256):
            scores = lax.dot_general(
                cols[pl.ds(base + part * 256, 256), :], side_block, NT, preferred_element_type=f32
            )
            squares = scores * scores
            adj[part * 256 : (part + 1) * 256, :] = (squares * squares * squares).astype(bf16)
        acc[:, pl.ds(side_at, TILE)] += jnp.dot(lt[...], adj[...], preferred_element_type=f32)

        ends = (LINE - 1) * TILES
        for after in range(1, TILES):

            @pl.when(t == ends + after)
            def _():
                to_partner(LINE - after).start()
                if after > 1:
                    pass_sum(LINE - after + 1)

        return carry

    lax.fori_loop(0, LINE * TILES, one_tile, 0)

    to_partner(0).wait_recv()
    conn = acc[:, pl.ds(pl.multiple_of(core * 256, 128), KEEP)] + pair[0]
    for chunk in range(1, LINE):
        remote(
            sent.at[chunk], got.at[chunk], send_sum.at[chunk], recv_sum.at[chunk], at_x(chunk)
        ).wait_recv()
        conn = conn + got[chunk].astype(f32)
    conn = jnp.where(core == 0, conn, pltpu.roll(conn, KEEP - 64, 1))

    which = lax.broadcasted_iota(jnp.int32, (KP, OWN), 0).astype(f32) - 150.0
    valid = conn[:, 0:OWN]
    kim = jnp.sum(jnp.where(which == own_ids[0:1, 0:OWN], valid, 0.0), axis=0, keepdims=True)
    rowsum = jnp.sum(valid, axis=0, keepdims=True)
    ref = ref_kim[...]
    stacked = jnp.concatenate(
        [kim, kim * kim, ref, ref * ref, kim * ref, rowsum, jnp.ones_like(kim), jnp.zeros_like(kim)],
        axis=0,
    )
    sums = jnp.dot(
        stacked, member[...], precision=lax.Precision.HIGHEST, preferred_element_type=f32
    )

    def wait_sent(copies):
        for copy in copies:
            copy.wait_send()

    place_xc = x * 2 + core
    sums_xc[place_xc] = sums
    copies = []
    for place in range(LINE):
        for flip in range(2):
            if place == 0 and flip == 0:
                continue
            peer = at_x(place, core if flip == 0 else other)
            copies.append((
                remote(
                    sums_xc.at[place_xc], sums_xc.at[place_xc], send_xc.at[place * 2 + flip],
                    recv_xc.at[SEEN_AS[place] * 2 + flip], peer,
                ),
                place, flip,
            ))
    for copy, _, _ in copies:
        copy.start()

    conn_out[...] = conn.T[0:OWN, 0:K]

    for copy, place, flip in copies:
        there = lax.rem(x + OFFSETS[place], LINE) * 2 + (core if flip == 0 else other)
        remote(
            sums_xc.at[there], sums_xc.at[there], send_xc.at[place * 2 + flip],
            recv_xc.at[place * 2 + flip], partner,
        ).wait_recv()
    total_sums = sums_xc[0]
    for index in range(1, 2 * LINE):
        total_sums = total_sums + sums_xc[index]
    wait_sent([copy for copy, _, _ in copies])

    for axis, (mine, buffer, at) in enumerate(((y, sums_y, at_y), (z, sums_z, at_z))):
        buffer[mine] = total_sums
        copies = []
        for place in range(1, LINE):
            copy = remote(
                buffer.at[mine], buffer.at[mine], send_yz.at[axis * LINE + place],
                recv_yz.at[axis * LINE + SEEN_AS[place]], at(place),
            )
            copy.start()
            copies.append(copy)
        for place in range(1, LINE):
            there = lax.rem(mine + OFFSETS[place], LINE)
            remote(
                buffer.at[there], buffer.at[there], send_yz.at[axis * LINE + place],
                recv_yz.at[axis * LINE + place], at(place),
            ).wait_recv()
        total_sums = buffer[0]
        for index in range(1, LINE):
            total_sums = total_sums + buffer[index]
        wait_sent(copies)

    s_k, s_kk, s_y, s_yy, s_ky, s_r, n = (total_sums[i : i + 1, 0:K] for i in range(7))
    mean_x = s_k / (n * n)
    var_x = jnp.maximum(s_kk / (n * n * n) - mean_x * mean_x, 0.0001)
    mean_y = s_y / n
    var_y = jnp.maximum(s_yy / n - mean_y * mean_y, 0.01)
    cross = s_ky / (n * n) - mean_x * mean_y
    between = (s_r - s_k) / (n * (float(G) - n))
    pres_out[0:1, :] = (mean_x - between) * jnp.sqrt(n / var_x)
    pres_out[1:2, :] = cross * jnp.sqrt(n / (var_x * var_y))

    wait_sent(started)
    for chunk in range(1, LINE):
        block = row_block(chunk, core)
        remote(block, block, send_fwd.at[chunk], recv_fwd.at[chunk], partner).wait_send()
        to_owner(chunk).wait_send()
    for chunk in range(LINE):
        to_partner(chunk).wait_send()


def whole(depth, compact, collective, resample, expression, labels, ref_kim):
    f32, bf16 = jnp.float32, jnp.bfloat16
    dma = pltpu.SemaphoreType.DMA
    vmem = pl.BlockSpec(memory_space=pltpu.VMEM)
    scratch = [
        pltpu.VMEM((ROWS, depth), bf16),
        pltpu.VMEM((COLS, depth), bf16),
        pltpu.VMEM((KP, STEP), bf16),
        pltpu.VMEM((STEP, TILE), bf16),
        pltpu.VMEM((KP, ROWS), f32),
        pltpu.VMEM((LINE, KP, KEEP), f32),
        pltpu.VMEM((LINE, KP, KEEP), bf16),
        pltpu.VMEM((LINE, KP, KEEP), bf16),
        pltpu.VMEM((16, KEEP), f32),
        pltpu.VMEM((OWN, KEEP), f32),
        pltpu.VMEM((2 * LINE, 8, KEEP), f32),
        pltpu.VMEM((LINE, 8, KEEP), f32),
        pltpu.VMEM((LINE, 8, KEEP), f32),
    ]
    for count in (LINE, LINE, 2 * LINE, 2 * LINE * LINE, LINE, LINE, 2 * LINE, 2 * LINE):
        scratch += [dma((count,)), dma((count,))]
    return pl.pallas_call(
        functools.partial(kernel, depth, compact),
        out_shape=(
            jax.ShapeDtypeStruct((OWN, K), f32),
            jax.ShapeDtypeStruct((2, K), f32),
        ),
        in_specs=[vmem] * 4,
        out_specs=(vmem, vmem),
        scratch_shapes=scratch,
        compiler_params=pltpu.CompilerParams(
            collective_id=collective, has_side_effects=True, vmem_limit_bytes=60 * 1024 * 1024
        ),
        name=f"network_{depth}",
    )(resample, expression, labels, ref_kim)


def local(expression, resample, labels, ref_kim):
    samples = jnp.arange(SAMPLES, dtype=jnp.int32)
    distinct = jnp.sum(jnp.any(resample[:, None] == samples[None, :], axis=0).astype(jnp.int32))
    return lax.cond(
        distinct <= 255,
        functools.partial(whole, 256, True, 0),
        functools.partial(whole, 512, False, 1),
        resample.reshape(1, SAMPLES),
        expression,
        labels,
        ref_kim.reshape(1, OWN),
    )


def solution(mesh):
    torus = Mesh(mesh.devices.reshape(4, 4, 2, 2, 2), AXES)
    placed = (P(None, AXES), P(), P(AXES, None), P(AXES))
    return jax.shard_map(
        local, mesh=torus, in_specs=placed, out_specs=(P(AXES, None), P()), check_vma=False
    )
```

```python
import functools

import jax
import jax.numpy as jnp
from jax import lax
from jax.experimental import pallas as pl
from jax.experimental.pallas import tpu as pltpu
from jax.sharding import Mesh
from jax.sharding import PartitionSpec as P

G = 40960
SAMPLES = 384
K = 300
KP = 304
OWN = 320
HALF = OWN // 2
LINE = 4
CHUNK = 2 * OWN
STEP = 2 * LINE * HALF
ROWS = LINE * CHUNK
COLS = LINE * STEP
TILE = 512
TILES = ROWS // TILE
KEEP = 384
AXES = ("z", "y", "xh", "c", "xl")
OFFSETS = (0, 1, 3, 2)
SEEN_AS = (0, 2, 1, 3)
NT = (((1,), (1,)), ((), ()))


def kernel(
    depth, compact, resample, expression, labels, ref_kim, conn_out, pres_out, count_out,
    rows, cols, lt, adj, acc, pair, sent, got, info, side_ids, side_lt, kim_rows, parts, stats,
    sums_y, sums_z,
    send_rows, recv_rows, send_fwd, recv_fwd, send_near, recv_near, send_far, recv_far,
    send_pair, recv_pair, send_sum, recv_sum, send_info, recv_info, send_part, recv_part,
    send_yz, recv_yz,
):
    f32, bf16 = jnp.float32, jnp.bfloat16
    z, y, core = lax.axis_index("z"), lax.axis_index("y"), lax.axis_index("c")
    x = lax.axis_index("xh") * 2 + lax.axis_index("xl")
    other = 1 - core

    def at_x(place, c=None):
        there = lax.rem(x + OFFSETS[place], LINE)
        device = {"xh": there // 2, "xl": lax.rem(there, 2)}
        if c is not None:
            device["c"] = c
        return device

    def at_y(place):
        return {"y": lax.rem(y + OFFSETS[place], LINE)}

    def at_z(place):
        return {"z": lax.rem(z + OFFSETS[place], LINE)}

    partner = {"c": other}

    barrier = pltpu.get_barrier_semaphore()
    peers = [partner]
    for place in range(1, LINE):
        peers += [at_x(place), at_x(place, other), at_y(place), at_z(place)]
    for peer in peers:
        pl.semaphore_signal(barrier, inc=1, device_id=peer, device_id_type=pl.DeviceIdType.MESH)

    def remote(src, dst, send_sem, recv_sem, device):
        return pltpu.make_async_remote_copy(
            src_ref=src, dst_ref=dst, send_sem=send_sem, recv_sem=recv_sem,
            device_id=device, device_id_type=pl.DeviceIdType.MESH,
        )

    started = []

    def send(*args):
        copy = remote(*args)
        copy.start()
        started.append(copy)

    sample = lax.broadcasted_iota(jnp.int32, (SAMPLES, SAMPLES), 0)
    hits = jnp.where(sample == resample[...], 1.0, 0.0).astype(bf16)
    times = lax.dot_general(
        jnp.ones((16, SAMPLES), bf16), hits, NT, preferred_element_type=f32
    )
    present = jnp.where(times > 0.5, 1.0, 0.0)
    if compact:
        before = jnp.where(
            sample < lax.broadcasted_iota(jnp.int32, (SAMPLES, SAMPLES), 1), 1.0, 0.0
        ).astype(bf16)
        rank = jnp.dot(present.astype(bf16), before, preferred_element_type=f32)
        place_of = jnp.where(present > 0.5, rank, -1.0)[0:1, :].astype(jnp.int32)
    else:
        place_of = lax.broadcasted_iota(jnp.int32, (1, SAMPLES), 1)
    count_out[0] = jnp.sum(present[0:1, :].astype(jnp.int32))
    times = times[0:1, :]
    pick = jnp.where(
        lax.broadcasted_iota(jnp.int32, (depth, SAMPLES), 0) == place_of, 1.0, 0.0
    ).astype(bf16)
    values = expression[...]
    mean = jnp.sum(values * times, axis=1, keepdims=True) * (1.0 / SAMPLES)
    centered = values - mean
    total = jnp.sum(centered * centered * times, axis=1, keepdims=True)
    scaled = (centered * lax.rsqrt(total + 1e-06)).astype(bf16)
    weighted = (scaled.astype(f32) * times).astype(bf16)
    side = lax.dot_general(weighted, pick, NT, preferred_element_type=f32)
    front = lax.dot_general(scaled, pick, NT, preferred_element_type=f32)
    marks = labels[...].astype(f32)
    module = lax.broadcasted_iota(jnp.int32, (K, depth), 0).astype(f32) - 150.0
    module = jnp.where(lax.broadcasted_iota(jnp.int32, (K, depth), 1) == depth - 1, module, 0.0)
    front = front + lax.dot_general(
        marks.astype(bf16), module.astype(bf16), (((0,), (0,)), ((), ())),
        preferred_element_type=f32,
    )
    front = front.astype(bf16)
    rows[pl.ds(pl.multiple_of(core * OWN, OWN), OWN), :] = side.astype(bf16)
    cols[0:HALF, :] = front[0:HALF]
    cols[STEP // 2 : STEP // 2 + HALF, :] = front[HALF:OWN]
    place_xc = x * 2 + core
    module = lax.broadcasted_iota(jnp.int32, (K, OWN), 0).astype(f32) - 150.0
    info[place_xc, 0:1, :] = jnp.full((1, KEEP), -1000.0, f32)
    info[place_xc, 1:2, :] = jnp.zeros((1, KEEP), f32)
    info[place_xc, 0:1, 0:OWN] = jnp.sum(marks * module, axis=0, keepdims=True)
    info[place_xc, 1:2, 0:OWN] = ref_kim[...]

    pl.semaphore_wait(barrier, len(peers))

    def row_block(chunk, c):
        return rows.at[pl.ds(pl.multiple_of(chunk * CHUNK + c * OWN, OWN), OWN), :]

    def col_block(step, part, slot):
        return cols.at[pl.ds(step * STEP + part * (STEP // 2) + slot * HALF, HALF), :]

    def near_index(part, place):
        return part * LINE + place

    def far_index(part, step, slot):
        return (part * LINE + step) * LINE + slot

    along = (at_z, at_y)
    across = (at_y, at_z)

    def group(place, flip):
        if place == 0:
            return partner
        return at_x(place) if flip == 0 else at_x(place, other)

    mates = [(0, 1)] + [(place, flip) for place in range(1, LINE) for flip in range(2)]

    def to_mates(buffer, send_sem, recv_sem):
        for place, flip in mates:
            send(
                buffer.at[place_xc], buffer.at[place_xc], send_sem.at[place * 2 + flip],
                recv_sem.at[SEEN_AS[place] * 2 + flip], group(place, flip),
            )

    def from_mates(buffer, send_sem, recv_sem):
        for place, flip in mates:
            there = lax.rem(x + OFFSETS[place], LINE) * 2 + (core if flip == 0 else other)
            remote(
                buffer.at[there], buffer.at[there], send_sem.at[place * 2 + flip],
                recv_sem.at[place * 2 + flip], group(place, flip),
            ).wait_recv()

    def forward_columns(part, slot, places):
        for place in places:
            send(
                col_block(0, part, slot), col_block(SEEN_AS[place], part, slot),
                send_far.at[far_index(part, place, slot)],
                recv_far.at[far_index(part, SEEN_AS[place], slot)], across[part](place),
            )

    to_mates(info, send_info, recv_info)
    send(row_block(0, core), row_block(0, core), send_fwd.at[0], recv_fwd.at[0], partner)
    for place in range(1, LINE):
        for part in range(2):
            send(
                col_block(0, part, 0), col_block(0, part, SEEN_AS[place]),
                send_near.at[near_index(part, place)],
                recv_near.at[near_index(part, SEEN_AS[place])], along[part](place),
            )
        send(
            row_block(0, core), row_block(SEEN_AS[place], core),
            send_rows.at[place], recv_rows.at[SEEN_AS[place]], at_x(place),
        )

    def wait_near(part, place):
        block = col_block(0, part, place)
        remote(
            block, block, send_near.at[near_index(part, place)],
            recv_near.at[near_index(part, place)], along[part](place),
        ).wait_recv()

    def wait_far(step):
        for part in range(2):
            for slot in range(LINE):
                block = col_block(step, part, slot)
                remote(
                    block, block, send_far.at[far_index(part, step, slot)],
                    recv_far.at[far_index(part, step, slot)], across[part](step),
                ).wait_recv()

    def pass_rows(chunk):
        block = row_block(chunk, core)
        remote(block, block, send_rows.at[chunk], recv_rows.at[chunk], at_x(chunk)).wait_recv()
        copy = remote(block, block, send_fwd.at[chunk], recv_fwd.at[chunk], partner)
        copy.start()

    def wait_rows(chunk):
        block = row_block(chunk, other)
        remote(block, block, send_fwd.at[chunk], recv_fwd.at[chunk], partner).wait_recv()

    for part in range(2):
        forward_columns(part, 0, (1, 2))

    acc[...] = jnp.zeros_like(acc)
    for place in range(1, LINE - 1):
        for part in range(2):
            wait_near(part, place)
            forward_columns(part, place, (1, 2))
    from_mates(info, send_info, recv_info)
    which = lax.broadcasted_iota(jnp.int32, (KP, KEEP), 0).astype(f32) - 150.0
    for index in range(2 * LINE):
        side_lt[:, index * KEEP : (index + 1) * KEEP] = jnp.where(
            which == info[index, 0:1, :], 1.0, 0.0
        ).astype(bf16)
    blank = jnp.zeros((1, CHUNK - KEEP), f32)
    for chunk in range(LINE):
        there = lax.rem(x + OFFSETS[chunk], LINE) * 2
        first = jnp.concatenate([info[there, 0:1, :] + 1000.0, blank], axis=1)
        second = jnp.concatenate([info[there + 1, 0:1, :] + 1000.0, blank], axis=1)
        both = first + pltpu.roll(second, OWN, 1) - 1000.0
        side_ids[0:1, chunk * CHUNK : (chunk + 1) * CHUNK] = both
    pass_rows(1)
    pass_rows(2)
    for part in range(2):
        wait_near(part, LINE - 1)
        forward_columns(part, LINE - 1, (1, 2))
    for slot in range(LINE):
        for part in range(2):
            forward_columns(part, slot, (LINE - 1,))
    wait_rows(0)

    def pair_slice(chunk, c):
        return acc.at[:, pl.ds(pl.multiple_of(chunk * CHUNK + c * 256, 128), KEEP)]

    def to_partner(chunk):
        return remote(
            pair_slice(chunk, other), pair.at[chunk], send_pair.at[chunk], recv_pair.at[chunk],
            partner,
        )

    def to_owner(chunk):
        return remote(
            sent.at[chunk], got.at[SEEN_AS[chunk]], send_sum.at[chunk],
            recv_sum.at[SEEN_AS[chunk]], at_x(chunk),
        )

    def pass_sum(chunk):
        to_partner(chunk).wait_recv()
        mine = acc[:, pl.ds(pl.multiple_of(chunk * CHUNK + core * 256, 128), KEEP)]
        sent[chunk] = (mine + pair[chunk]).astype(bf16)
        to_owner(chunk).start()

    def one_tile(t, carry):
        step, turn = t // TILES, lax.rem(t, TILES)
        tile = jnp.where(step == LINE - 1, TILES - 1 - turn, turn)
        base = pl.multiple_of(step * STEP, STEP)
        side_at = pl.multiple_of(tile * TILE, TILE)

        @pl.when(t == 1)
        def _():
            wait_rows(1)

        @pl.when(t == 2)
        def _():
            pass_rows(3)
            wait_rows(2)

        @pl.when(t == 3)
        def _():
            wait_rows(3)

        for far in range(1, LINE):

            @pl.when(t == far * TILES)
            def _():
                wait_far(far)

        @pl.when(turn == 0)
        def _():
            last = lax.broadcasted_iota(jnp.int32, (16, depth), 1) == depth - 1
            ids = lax.dot_general(
                jnp.where(last, 1.0, 0.0).astype(bf16), cols[pl.ds(base, STEP), :], NT,
                preferred_element_type=f32,
            )
            which = lax.broadcasted_iota(jnp.int32, (KP, STEP), 0).astype(f32) - 150.0
            lt[...] = jnp.where(which == ids[0:1, :], 1.0, 0.0).astype(bf16)

        side_block = rows[pl.ds(side_at, TILE), :]
        for part in range(STEP // 256):
            scores = lax.dot_general(
                cols[pl.ds(base + part * 256, 256), :], side_block, NT, preferred_element_type=f32
            )
            squares = scores * scores
            adj[part * 256 : (part + 1) * 256, :] = (squares * squares * squares).astype(bf16)
        acc[:, pl.ds(side_at, TILE)] += jnp.dot(lt[...], adj[...], preferred_element_type=f32)

        ends = (LINE - 1) * TILES

        @pl.when(t >= ends)
        def _():
            which = lax.broadcasted_iota(jnp.int32, (KP, TILE), 0).astype(f32) - 150.0
            done = acc[:, pl.ds(side_at, TILE)]
            hit = which == side_ids[0:1, pl.ds(side_at, TILE)]
            kim_rows[0:1, pl.ds(side_at, TILE)] = jnp.sum(
                jnp.where(hit, done, 0.0), axis=0, keepdims=True
            )
            kim_rows[1:2, pl.ds(side_at, TILE)] = jnp.sum(done, axis=0, keepdims=True)

        for after in range(1, TILES):

            @pl.when(t == ends + after)
            def _():
                to_partner(LINE - after).start()

        return carry

    lax.fori_loop(0, LINE * TILES, one_tile, 0)

    for chunk in range(LINE):
        there = lax.rem(x + OFFSETS[chunk], LINE) * 2
        for c in range(2):
            for kind in range(2):
                piece = kim_rows[kind : kind + 1, chunk * CHUNK + c * 256 : chunk * CHUNK + c * 256 + KEEP]
                if c == 1:
                    piece = pltpu.roll(piece, KEEP - 64, 1)
                parts[place_xc, kind, pl.ds(there + c, 1), :] = piece
    to_mates(parts, send_part, recv_part)
    for chunk in range(LINE - 1, 0, -1):
        pass_sum(chunk)

    from_mates(parts, send_part, recv_part)
    kim, rowsum = parts[0, 0], parts[0, 1]
    for index in range(1, 2 * LINE):
        kim = kim + parts[index, 0]
        rowsum = rowsum + parts[index, 1]
    for index in range(2 * LINE):
        at = slice(index * KEEP, (index + 1) * KEEP)
        k, r, ref = kim[index : index + 1], rowsum[index : index + 1], info[index, 1:2, :]
        one, none = jnp.ones_like(k), jnp.zeros_like(k)
        stats[:, at] = jnp.concatenate([k, k * k, ref, ref * ref, k * ref, r, one, none], axis=0)
    exact = stats[...]
    high = exact.astype(bf16).astype(f32)
    middle = (exact - high).astype(bf16).astype(f32)
    low = exact - high - middle
    split = jnp.concatenate([high, middle, low, jnp.zeros_like(low)], axis=0).astype(bf16)
    sums = lax.dot_general(split, side_lt[...], NT, preferred_element_type=f32)
    total_sums = sums[0:8] + sums[8:16] + sums[16:24]

    def wait_sent(copies):
        for copy in copies:
            copy.wait_send()

    for axis, (mine, buffer, at) in enumerate(((y, sums_y, at_y), (z, sums_z, at_z))):
        buffer[mine] = total_sums
        copies = []
        for place in range(1, LINE):
            copy = remote(
                buffer.at[mine], buffer.at[mine], send_yz.at[axis * LINE + place],
                recv_yz.at[axis * LINE + SEEN_AS[place]], at(place),
            )
            copy.start()
            copies.append(copy)
        for place in range(1, LINE):
            there = lax.rem(mine + OFFSETS[place], LINE)
            remote(
                buffer.at[there], buffer.at[there], send_yz.at[axis * LINE + place],
                recv_yz.at[axis * LINE + place], at(place),
            ).wait_recv()
        total_sums = buffer[0]
        for index in range(1, LINE):
            total_sums = total_sums + buffer[index]
        wait_sent(copies)

    s_k, s_kk, s_y, s_yy, s_ky, s_r, n = (total_sums[i : i + 1, 0:K] for i in range(7))
    mean_x = s_k / (n * n)
    var_x = jnp.maximum(s_kk / (n * n * n) - mean_x * mean_x, 0.0001)
    mean_y = s_y / n
    var_y = jnp.maximum(s_yy / n - mean_y * mean_y, 0.01)
    cross = s_ky / (n * n) - mean_x * mean_y
    between = (s_r - s_k) / (n * (float(G) - n))
    pres_out[0:1, :] = (mean_x - between) * jnp.sqrt(n / var_x)
    pres_out[1:2, :] = cross * jnp.sqrt(n / (var_x * var_y))

    to_partner(0).wait_recv()
    conn = acc[:, pl.ds(pl.multiple_of(core * 256, 128), KEEP)] + pair[0]
    for chunk in range(1, LINE):
        remote(
            sent.at[chunk], got.at[chunk], send_sum.at[chunk], recv_sum.at[chunk], at_x(chunk)
        ).wait_recv()
        conn = conn + got[chunk].astype(f32)
    conn = jnp.where(core == 0, conn, pltpu.roll(conn, KEEP - 64, 1))
    conn_out[...] = conn[0:K, 0:OWN]

    wait_sent(started)
    for chunk in range(1, LINE):
        block = row_block(chunk, core)
        remote(block, block, send_fwd.at[chunk], recv_fwd.at[chunk], partner).wait_send()
        to_owner(chunk).wait_send()
    for chunk in range(LINE):
        to_partner(chunk).wait_send()


def whole(depth, compact, collective, resample, expression, labels, ref_kim):
    f32, bf16 = jnp.float32, jnp.bfloat16
    dma = pltpu.SemaphoreType.DMA
    vmem = pl.BlockSpec(memory_space=pltpu.VMEM)
    scratch = [
        pltpu.VMEM((ROWS, depth), bf16),
        pltpu.VMEM((COLS, depth), bf16),
        pltpu.VMEM((KP, STEP), bf16),
        pltpu.VMEM((STEP, TILE), bf16),
        pltpu.VMEM((KP, ROWS), f32),
        pltpu.VMEM((LINE, KP, KEEP), f32),
        pltpu.VMEM((LINE, KP, KEEP), bf16),
        pltpu.VMEM((LINE, KP, KEEP), bf16),
        pltpu.VMEM((2 * LINE, 2, KEEP), f32),
        pltpu.VMEM((8, ROWS), f32),
        pltpu.VMEM((KP, 2 * LINE * KEEP), bf16),
        pltpu.VMEM((8, ROWS), f32),
        pltpu.VMEM((2 * LINE, 2, 2 * LINE, KEEP), f32),
        pltpu.VMEM((8, 2 * LINE * KEEP), f32),
        pltpu.VMEM((LINE, 8, KP), f32),
        pltpu.VMEM((LINE, 8, KP), f32),
    ]
    for count in (
        LINE, LINE, 2 * LINE, 2 * LINE * LINE, LINE, LINE, 2 * LINE, 2 * LINE, 2 * LINE,
    ):
        scratch += [dma((count,)), dma((count,))]
    return pl.pallas_call(
        functools.partial(kernel, depth, compact),
        out_shape=(
            jax.ShapeDtypeStruct((K, OWN), f32),
            jax.ShapeDtypeStruct((2, K), f32),
            jax.ShapeDtypeStruct((1,), jnp.int32),
        ),
        in_specs=[vmem] * 4,
        out_specs=(vmem, vmem, pl.BlockSpec(memory_space=pltpu.SMEM)),
        scratch_shapes=scratch,
        compiler_params=pltpu.CompilerParams(
            collective_id=collective, has_side_effects=True, vmem_limit_bytes=60 * 1024 * 1024
        ),
        name=f"network_{depth}",
    )(resample, expression, labels, ref_kim)


def local(expression, resample, labels, ref_kim):
    operands = (
        resample.reshape(1, SAMPLES), expression.T, labels.T, ref_kim.reshape(1, OWN),
    )
    conn, preservation, distinct = whole(256, True, 0, *operands)
    conn, preservation = lax.cond(
        distinct[0] <= 255,
        lambda *ready: ready[:2],
        lambda *ready: whole(512, False, 1, *ready[2:])[:2],
        conn, preservation, *operands,
    )
    return conn.T, preservation


def solution(mesh):
    torus = Mesh(mesh.devices.reshape(4, 4, 2, 2, 2), AXES)
    placed = (P(None, AXES), P(), P(AXES, None), P(AXES))
    return jax.shard_map(
        local, mesh=torus, in_specs=placed, out_specs=(P(AXES, None), P()), check_vma=False
    )
```

```python
import functools

import jax
import jax.numpy as jnp
from jax import lax
from jax.experimental import pallas as pl
from jax.experimental.pallas import tpu as pltpu
from jax.sharding import Mesh
from jax.sharding import PartitionSpec as P

G = 40960
SAMPLES = 384
K = 300
KP = 304
OWN = 320
HALF = OWN // 2
LINE = 4
CHUNK = 2 * OWN
EARLY = 2 * (LINE - 1) * HALF
LATE = 2 * LINE * HALF
ROWS = LINE * CHUNK
COLS = LINE * EARLY + LATE
TILE = 512
TILES = ROWS // TILE
KEEP = 384
AXES = ("z", "y", "xh", "c", "xl")
OFFSETS = (0, 1, 3, 2)
SEEN_AS = (0, 2, 1, 3)
NT = (((1,), (1,)), ((), ()))


def kernel(
    depth, compact, resample, expression, labels, ref_kim, conn_out, pres_out, count_out,
    values_in, labels_in, rows, cols, lt, lt_late, even, odd, acc, pair, sent, got, info, side_ids, side_lt,
    kim_rows, parts, stats, sums_y, sums_z, loaded,
    send_rows, recv_rows, send_fwd, recv_fwd, send_near, recv_near, send_far, recv_far,
    send_pair, recv_pair, send_sum, recv_sum, send_info, recv_info, send_part, recv_part,
    send_yz, recv_yz,
):
    f32, bf16 = jnp.float32, jnp.bfloat16
    z, y, core = lax.axis_index("z"), lax.axis_index("y"), lax.axis_index("c")
    x = lax.axis_index("xh") * 2 + lax.axis_index("xl")
    other = 1 - core

    def at_x(place, c=None):
        there = lax.rem(x + OFFSETS[place], LINE)
        device = {"xh": there // 2, "xl": lax.rem(there, 2)}
        if c is not None:
            device["c"] = c
        return device

    def at_y(place):
        return {"y": lax.rem(y + OFFSETS[place], LINE)}

    def at_z(place):
        return {"z": lax.rem(z + OFFSETS[place], LINE)}

    partner = {"c": other}

    load_values = pltpu.make_async_copy(expression, values_in, loaded.at[0])
    load_labels = pltpu.make_async_copy(labels, labels_in, loaded.at[1])
    load_values.start()
    load_labels.start()
    barrier = pltpu.get_barrier_semaphore()
    peers = [partner]
    for place in range(1, LINE):
        peers += [at_x(place), at_x(place, other), at_y(place), at_z(place)]
    for peer in peers:
        pl.semaphore_signal(barrier, inc=1, device_id=peer, device_id_type=pl.DeviceIdType.MESH)

    def remote(src, dst, send_sem, recv_sem, device):
        return pltpu.make_async_remote_copy(
            src_ref=src, dst_ref=dst, send_sem=send_sem, recv_sem=recv_sem,
            device_id=device, device_id_type=pl.DeviceIdType.MESH,
        )

    started = []

    def send(*args):
        copy = remote(*args)
        copy.start()
        started.append(copy)

    sample = lax.broadcasted_iota(jnp.int32, (SAMPLES, SAMPLES), 0)
    hits = jnp.where(sample == resample[...], 1.0, 0.0).astype(bf16)
    times = lax.dot_general(
        jnp.ones((16, SAMPLES), bf16), hits, NT, preferred_element_type=f32
    )
    present = jnp.where(times > 0.5, 1.0, 0.0)
    if compact:
        before = jnp.where(
            sample < lax.broadcasted_iota(jnp.int32, (SAMPLES, SAMPLES), 1), 1.0, 0.0
        ).astype(bf16)
        rank = jnp.dot(present.astype(bf16), before, preferred_element_type=f32)
        place_of = jnp.where(present > 0.5, rank, -1.0)[0:1, :].astype(jnp.int32)
    else:
        place_of = lax.broadcasted_iota(jnp.int32, (1, SAMPLES), 1)
    count_out[0] = jnp.sum(present[0:1, :].astype(jnp.int32))
    times = times[0:1, :]
    pick = jnp.where(
        lax.broadcasted_iota(jnp.int32, (depth, SAMPLES), 0) == place_of, 1.0, 0.0
    ).astype(bf16)
    load_values.wait()
    values = values_in[...]
    mean = jnp.sum(values * times, axis=1, keepdims=True) * (1.0 / SAMPLES)
    centered = values - mean
    total = jnp.sum(centered * centered * times, axis=1, keepdims=True)
    scaled = (centered * lax.rsqrt(total + 1e-06)).astype(bf16)
    weighted = (scaled.astype(f32) * times).astype(bf16)
    side = lax.dot_general(weighted, pick, NT, preferred_element_type=f32)
    front = lax.dot_general(scaled, pick, NT, preferred_element_type=f32)
    load_labels.wait()
    marks = labels_in[...].astype(f32)
    module = lax.broadcasted_iota(jnp.int32, (K, depth), 0).astype(f32) - 150.0
    module = jnp.where(lax.broadcasted_iota(jnp.int32, (K, depth), 1) == depth - 1, module, 0.0)
    front = front + lax.dot_general(
        marks.astype(bf16), module.astype(bf16), (((0,), (0,)), ((), ())),
        preferred_element_type=f32,
    )
    front = front.astype(bf16)
    rows[pl.ds(pl.multiple_of(core * OWN, OWN), OWN), :] = side.astype(bf16)
    cols[0:HALF, :] = front[0:HALF]
    cols[EARLY // 2 : EARLY // 2 + HALF, :] = front[HALF:OWN]
    place_xc = x * 2 + core
    module = lax.broadcasted_iota(jnp.int32, (K, OWN), 0).astype(f32) - 150.0
    info[place_xc, 0:1, :] = jnp.full((1, KEEP), -1000.0, f32)
    info[place_xc, 1:2, :] = jnp.zeros((1, KEEP), f32)
    info[place_xc, 0:1, 0:OWN] = jnp.sum(marks * module, axis=0, keepdims=True)
    info[place_xc, 1:2, 0:OWN] = ref_kim[...]

    pl.semaphore_wait(barrier, len(peers))

    def row_block(chunk, c):
        return rows.at[pl.ds(pl.multiple_of(chunk * CHUNK + c * OWN, OWN), OWN), :]

    def col_block(step, part, slot):
        if step == LINE - 1:
            at = LINE * EARLY + part * (LATE // 2) + slot * HALF
        elif slot == LINE - 1:
            at = (LINE - 1) * EARLY + step * OWN + part * HALF
        else:
            at = step * EARLY + part * (EARLY // 2) + slot * HALF
        return cols.at[pl.ds(at, HALF), :]

    def near_index(part, place):
        return part * LINE + place

    def far_index(part, step, slot):
        return (part * LINE + step) * LINE + slot

    along = (at_z, at_y)
    across = (at_y, at_z)

    def group(place, flip):
        if place == 0:
            return partner
        return at_x(place) if flip == 0 else at_x(place, other)

    mates = [(0, 1)] + [(place, flip) for place in range(1, LINE) for flip in range(2)]

    def to_mates(buffer, send_sem, recv_sem):
        for place, flip in mates:
            send(
                buffer.at[place_xc], buffer.at[place_xc], send_sem.at[place * 2 + flip],
                recv_sem.at[SEEN_AS[place] * 2 + flip], group(place, flip),
            )

    def from_mates(buffer, send_sem, recv_sem):
        for place, flip in mates:
            there = lax.rem(x + OFFSETS[place], LINE) * 2 + (core if flip == 0 else other)
            remote(
                buffer.at[there], buffer.at[there], send_sem.at[place * 2 + flip],
                recv_sem.at[place * 2 + flip], group(place, flip),
            ).wait_recv()

    def far_copy(part, slot, place):
        return remote(
            col_block(0, part, slot), col_block(SEEN_AS[place], part, slot),
            send_far.at[far_index(part, place, slot)],
            recv_far.at[far_index(part, SEEN_AS[place], slot)], across[part](place),
        )

    def forward_columns(part, slot, places):
        for place in places:
            far_copy(part, slot, place).start()

    def send_near_columns(place):
        for part in range(2):
            send(
                col_block(0, part, 0), col_block(0, part, SEEN_AS[place]),
                send_near.at[near_index(part, place)],
                recv_near.at[near_index(part, SEEN_AS[place])], along[part](place),
            )

    for place in range(1, LINE):
        if place < LINE - 1:
            send_near_columns(place)
        send(
            row_block(0, core), row_block(SEEN_AS[place], core),
            send_rows.at[place], recv_rows.at[SEEN_AS[place]], at_x(place),
        )
        if place == 1:
            send(row_block(0, core), row_block(0, core), send_fwd.at[0], recv_fwd.at[0], partner)
    to_mates(info, send_info, recv_info)

    def wait_near(part, place):
        block = col_block(0, part, place)
        remote(
            block, block, send_near.at[near_index(part, place)],
            recv_near.at[near_index(part, place)], along[part](place),
        ).wait_recv()

    def wait_far(step, slots):
        for part in range(2):
            for slot in slots:
                block = col_block(step, part, slot)
                remote(
                    block, block, send_far.at[far_index(part, step, slot)],
                    recv_far.at[far_index(part, step, slot)], across[part](step),
                ).wait_recv()

    def pass_rows(chunk):
        block = row_block(chunk, core)
        remote(block, block, send_rows.at[chunk], recv_rows.at[chunk], at_x(chunk)).wait_recv()
        copy = remote(block, block, send_fwd.at[chunk], recv_fwd.at[chunk], partner)
        copy.start()

    def wait_rows(chunk):
        block = row_block(chunk, other)
        remote(block, block, send_fwd.at[chunk], recv_fwd.at[chunk], partner).wait_recv()

    for part in range(2):
        forward_columns(part, 0, (1, 2))

    acc[...] = jnp.zeros_like(acc)
    for place in range(1, LINE - 1):
        for part in range(2):
            wait_near(part, place)
            forward_columns(part, place, (1, 2))
    send_near_columns(LINE - 1)
    for slot in range(LINE - 1):
        for part in range(2):
            forward_columns(part, slot, (LINE - 1,))
    wait_rows(0)

    def take_info():
        from_mates(info, send_info, recv_info)
        which = lax.broadcasted_iota(jnp.int32, (KP, KEEP), 0).astype(f32) - 150.0
        for index in range(2 * LINE):
            side_lt[:, index * KEEP : (index + 1) * KEEP] = jnp.where(
                which == info[index, 0:1, :], 1.0, 0.0
            ).astype(bf16)
        blank = jnp.zeros((1, CHUNK - KEEP), f32)
        for chunk in range(LINE):
            there = lax.rem(x + OFFSETS[chunk], LINE) * 2
            first = jnp.concatenate([info[there, 0:1, :] + 1000.0, blank], axis=1)
            second = jnp.concatenate([info[there + 1, 0:1, :] + 1000.0, blank], axis=1)
            both = first + pltpu.roll(second, OWN, 1) - 1000.0
            side_ids[0:1, chunk * CHUNK : (chunk + 1) * CHUNK] = both

    def pair_slice(chunk, c):
        return acc.at[:, pl.ds(pl.multiple_of(chunk * CHUNK + c * 256, 128), KEEP)]

    def to_partner(chunk):
        return remote(
            pair_slice(chunk, other), pair.at[chunk], send_pair.at[chunk], recv_pair.at[chunk],
            partner,
        )

    def to_owner(chunk):
        return remote(
            sent.at[chunk], got.at[SEEN_AS[chunk]], send_sum.at[chunk],
            recv_sum.at[SEEN_AS[chunk]], at_x(chunk),
        )

    def pass_sum(chunk):
        to_partner(chunk).wait_recv()
        mine = acc[:, pl.ds(pl.multiple_of(chunk * CHUNK + core * 256, 128), KEEP)]
        sent[chunk] = (mine + pair[chunk]).astype(bf16)
        to_owner(chunk).start()

    def make_labels(base, width):
        last = lax.broadcasted_iota(jnp.int32, (16, depth), 1) == depth - 1
        ids = lax.dot_general(
            jnp.where(last, 1.0, 0.0).astype(bf16), cols[pl.ds(base, width), :], NT,
            preferred_element_type=f32,
        )
        which = lax.broadcasted_iota(jnp.int32, (KP, width), 0).astype(f32) - 150.0
        return jnp.where(which == ids[0:1, :], 1.0, 0.0).astype(bf16)

    def score(into, base, width, side_at):
        side_block = rows[pl.ds(side_at, TILE), :]
        for start in range(0, width, 256):
            size = min(256, width - start)
            scores = lax.dot_general(
                cols[pl.ds(base + start, size), :], side_block, NT, preferred_element_type=f32
            )
            squares = scores * scores
            into[start : start + size, :] = (squares * squares * squares).astype(bf16)

    def count(held, width, side_at, module_rows):
        acc[:, pl.ds(side_at, TILE)] += jnp.dot(
            module_rows, held[0:width, :], preferred_element_type=f32
        )

    soon = (LINE - 1) * 3
    later = soon + (LINE - 1) * 2

    def task(t):
        group = jnp.where(
            t < soon, t // 3, jnp.where(t < later, (t - soon) // 2, LINE - 1)
        )
        tile = jnp.where(
            t < soon, lax.rem(t, 3), jnp.where(t < later, 3 + lax.rem(t + 1, 2), t - later)
        )
        return group, pl.multiple_of(group * EARLY, HALF), pl.multiple_of(tile * TILE, TILE)

    def score_task(into, t):
        group, base, side_at = task(t)
        score(into, base, EARLY, side_at)

    def count_task(held, t):
        group, base, side_at = task(t)
        count(held, EARLY, side_at, lt[group])

    lt[0] = make_labels(0, EARLY)
    score_task(even, 0)
    pass_rows(1)
    pass_rows(2)
    take_info()

    def two_tiles(u, carry):
        @pl.when(u == 0)
        def _():
            wait_rows(1)
            wait_rows(2)

        for far in range(1, LINE - 1):

            @pl.when(u == far)
            def _():
                wait_far(far, range(LINE - 1))
                lt[far] = make_labels(far * EARLY, EARLY)
                if far == LINE - 2:
                    for part in range(2):
                        wait_near(part, LINE - 1)
                        forward_columns(part, LINE - 1, (1, 2, 3))
                    pass_rows(3)

        @pl.when(u == (soon - 1) // 2)
        def _():
            wait_rows(3)

        @pl.when(u == (later - 1) // 2)
        def _():
            wait_far(1, (LINE - 1,))
            wait_far(2, (LINE - 1,))
            lt[LINE - 1] = make_labels((LINE - 1) * EARLY, EARLY)

        count_task(even, 2 * u)
        score_task(odd, 2 * u + 1)
        count_task(odd, 2 * u + 1)
        score_task(even, 2 * u + 2)
        return carry

    pairs = (later + TILES - 2) // 2
    lax.fori_loop(0, pairs, two_tiles, 0)
    count_task(even, 2 * pairs)
    score_task(odd, 2 * pairs + 1)
    wait_far(LINE - 1, range(LINE))
    lt_late[...] = make_labels(LINE * EARLY, LATE)
    count_task(odd, 2 * pairs + 1)
    score(even, LINE * EARLY, LATE, (TILES - 1) * TILE)
    for turn in range(TILES):
        side_at = (TILES - 1 - turn) * TILE
        held, into = (even, odd) if turn % 2 == 0 else (odd, even)
        count(held, LATE, side_at, lt_late[...])
        if turn < TILES - 1:
            score(into, LINE * EARLY, LATE, side_at - TILE)
        which = lax.broadcasted_iota(jnp.int32, (KP, TILE), 0).astype(f32) - 150.0
        done = acc[:, side_at : side_at + TILE]
        hit = which == side_ids[0:1, side_at : side_at + TILE]
        kim_rows[0:1, side_at : side_at + TILE] = jnp.sum(
            jnp.where(hit, done, 0.0), axis=0, keepdims=True
        )
        kim_rows[1:2, side_at : side_at + TILE] = jnp.sum(done, axis=0, keepdims=True)
        if turn > 0:
            to_partner(LINE - turn).start()

    for chunk in range(LINE):
        there = lax.rem(x + OFFSETS[chunk], LINE) * 2
        for c in range(2):
            for kind in range(2):
                piece = kim_rows[kind : kind + 1, chunk * CHUNK + c * 256 : chunk * CHUNK + c * 256 + KEEP]
                if c == 1:
                    piece = pltpu.roll(piece, KEEP - 64, 1)
                parts[place_xc, kind, pl.ds(there + c, 1), :] = piece
    to_mates(parts, send_part, recv_part)
    for chunk in range(LINE - 1, 0, -1):
        pass_sum(chunk)

    from_mates(parts, send_part, recv_part)
    kim, rowsum = parts[0, 0], parts[0, 1]
    for index in range(1, 2 * LINE):
        kim = kim + parts[index, 0]
        rowsum = rowsum + parts[index, 1]
    for index in range(2 * LINE):
        at = slice(index * KEEP, (index + 1) * KEEP)
        k, r, ref = kim[index : index + 1], rowsum[index : index + 1], info[index, 1:2, :]
        one, none = jnp.ones_like(k), jnp.zeros_like(k)
        stats[:, at] = jnp.concatenate([k, k * k, ref, ref * ref, k * ref, r, one, none], axis=0)
    exact = stats[...]
    high = exact.astype(bf16).astype(f32)
    middle = (exact - high).astype(bf16).astype(f32)
    low = exact - high - middle
    split = jnp.concatenate([high, middle, low, jnp.zeros_like(low)], axis=0).astype(bf16)
    sums = lax.dot_general(split, side_lt[...], NT, preferred_element_type=f32)
    total_sums = sums[0:8] + sums[8:16] + sums[16:24]

    def wait_sent(copies):
        for copy in copies:
            copy.wait_send()

    for axis, (mine, buffer, at) in enumerate(((y, sums_y, at_y), (z, sums_z, at_z))):
        buffer[mine] = total_sums
        copies = []
        for place in range(1, LINE):
            copy = remote(
                buffer.at[mine], buffer.at[mine], send_yz.at[axis * LINE + place],
                recv_yz.at[axis * LINE + SEEN_AS[place]], at(place),
            )
            copy.start()
            copies.append(copy)
        for place in range(1, LINE):
            there = lax.rem(mine + OFFSETS[place], LINE)
            remote(
                buffer.at[there], buffer.at[there], send_yz.at[axis * LINE + place],
                recv_yz.at[axis * LINE + place], at(place),
            ).wait_recv()
        total_sums = buffer[0]
        for index in range(1, LINE):
            total_sums = total_sums + buffer[index]
        wait_sent(copies)

    s_k, s_kk, s_y, s_yy, s_ky, s_r, n = (total_sums[i : i + 1, 0:K] for i in range(7))
    mean_x = s_k / (n * n)
    var_x = jnp.maximum(s_kk / (n * n * n) - mean_x * mean_x, 0.0001)
    mean_y = s_y / n
    var_y = jnp.maximum(s_yy / n - mean_y * mean_y, 0.01)
    cross = s_ky / (n * n) - mean_x * mean_y
    between = (s_r - s_k) / (n * (float(G) - n))
    pres_out[0:1, :] = (mean_x - between) * jnp.sqrt(n / var_x)
    pres_out[1:2, :] = cross * jnp.sqrt(n / (var_x * var_y))

    to_partner(0).wait_recv()
    conn = acc[:, pl.ds(pl.multiple_of(core * 256, 128), KEEP)] + pair[0]
    for chunk in range(1, LINE):
        remote(
            sent.at[chunk], got.at[chunk], send_sum.at[chunk], recv_sum.at[chunk], at_x(chunk)
        ).wait_recv()
        conn = conn + got[chunk].astype(f32)
    conn = jnp.where(core == 0, conn, pltpu.roll(conn, KEEP - 64, 1))
    conn_out[...] = conn[0:K, 0:OWN]

    wait_sent(started)
    for place in range(1, LINE):
        for part in range(2):
            for slot in range(LINE):
                far_copy(part, slot, place).wait_send()
    for chunk in range(1, LINE):
        block = row_block(chunk, core)
        remote(block, block, send_fwd.at[chunk], recv_fwd.at[chunk], partner).wait_send()
        to_owner(chunk).wait_send()
    for chunk in range(LINE):
        to_partner(chunk).wait_send()


def whole(depth, compact, collective, resample, expression, labels, ref_kim):
    f32, bf16 = jnp.float32, jnp.bfloat16
    dma = pltpu.SemaphoreType.DMA
    vmem, hbm = pl.BlockSpec(memory_space=pltpu.VMEM), pl.BlockSpec(memory_space=pl.ANY)
    scratch = [
        pltpu.VMEM((OWN, SAMPLES), f32),
        pltpu.VMEM((K, OWN), jnp.int32),
        pltpu.VMEM((ROWS, depth), bf16),
        pltpu.VMEM((COLS, depth), bf16),
        pltpu.VMEM((LINE, KP, EARLY), bf16),
        pltpu.VMEM((KP, LATE), bf16),
        pltpu.VMEM((LATE, TILE), bf16),
        pltpu.VMEM((LATE, TILE), bf16),
        pltpu.VMEM((KP, ROWS), f32),
        pltpu.VMEM((LINE, KP, KEEP), f32),
        pltpu.VMEM((LINE, KP, KEEP), bf16),
        pltpu.VMEM((LINE, KP, KEEP), bf16),
        pltpu.VMEM((2 * LINE, 2, KEEP), f32),
        pltpu.VMEM((8, ROWS), f32),
        pltpu.VMEM((KP, 2 * LINE * KEEP), bf16),
        pltpu.VMEM((8, ROWS), f32),
        pltpu.VMEM((2 * LINE, 2, 2 * LINE, KEEP), f32),
        pltpu.VMEM((8, 2 * LINE * KEEP), f32),
        pltpu.VMEM((LINE, 8, KP), f32),
        pltpu.VMEM((LINE, 8, KP), f32),
        dma((2,)),
    ]
    for count in (
        LINE, LINE, 2 * LINE, 2 * LINE * LINE, LINE, LINE, 2 * LINE, 2 * LINE, 2 * LINE,
    ):
        scratch += [dma((count,)), dma((count,))]
    return pl.pallas_call(
        functools.partial(kernel, depth, compact),
        out_shape=(
            jax.ShapeDtypeStruct((K, OWN), f32),
            jax.ShapeDtypeStruct((2, K), f32),
            jax.ShapeDtypeStruct((1,), jnp.int32),
        ),
        in_specs=[vmem, hbm, hbm, vmem],
        out_specs=(vmem, vmem, pl.BlockSpec(memory_space=pltpu.SMEM)),
        scratch_shapes=scratch,
        compiler_params=pltpu.CompilerParams(
            collective_id=collective, has_side_effects=True, vmem_limit_bytes=60 * 1024 * 1024
        ),
        name=f"network_{depth}",
    )(resample, expression, labels, ref_kim)


def local(expression, resample, labels, ref_kim):
    operands = (
        resample.reshape(1, SAMPLES), expression.T, labels.T, ref_kim.reshape(1, OWN),
    )
    conn, preservation, distinct = whole(256, True, 0, *operands)
    conn, preservation = lax.cond(
        distinct[0] <= 255,
        lambda *ready: ready[:2],
        lambda *ready: whole(512, False, 1, *ready[2:])[:2],
        conn, preservation, *operands,
    )
    return conn.T, preservation


def solution(mesh):
    torus = Mesh(mesh.devices.reshape(4, 4, 2, 2, 2), AXES)
    placed = (P(None, AXES), P(), P(AXES, None), P(AXES))
    return jax.shard_map(
        local, mesh=torus, in_specs=placed, out_specs=(P(AXES, None), P()), check_vma=False
    )
```

```python
import functools

import jax
import jax.numpy as jnp
from jax import lax
from jax.experimental import pallas as pl
from jax.experimental.pallas import tpu as pltpu
from jax.sharding import Mesh
from jax.sharding import PartitionSpec as P

G = 40960
SAMPLES = 384
K = 300
KP = 304
OWN = 320
HALF = OWN // 2
LINE = 4
CHUNK = 2 * OWN
EARLY = 2 * (LINE - 1) * HALF
LATE = 2 * LINE * HALF
ROWS = LINE * CHUNK
COLS = LINE * EARLY + LATE
TILE = 512
TILES = ROWS // TILE
KEEP = 384
AXES = ("z", "y", "xh", "c", "xl")
OFFSETS = (0, 1, 3, 2)
SEEN_AS = (0, 2, 1, 3)
NT = (((1,), (1,)), ((), ()))


def kernel(
    depth, compact, resample, expression, labels, ref_kim, conn_out, pres_out, count_out,
    values_in, labels_in, rows, cols, lt, lt_late, even, odd, acc, pair, sent, got, info, side_ids, side_lt,
    kim_rows, parts, stats, sums_y, sums_z, loaded,
    send_rows, recv_rows, send_fwd, recv_fwd, send_near, recv_near, send_far, recv_far,
    send_pair, recv_pair, send_sum, recv_sum, send_info, recv_info, send_part, recv_part,
    send_yz, recv_yz,
):
    f32, bf16 = jnp.float32, jnp.bfloat16
    z, y, core = lax.axis_index("z"), lax.axis_index("y"), lax.axis_index("c")
    x = lax.axis_index("xh") * 2 + lax.axis_index("xl")
    other = 1 - core

    def at_x(place, c=None):
        there = lax.rem(x + OFFSETS[place], LINE)
        device = {"xh": there // 2, "xl": lax.rem(there, 2)}
        if c is not None:
            device["c"] = c
        return device

    def at_y(place):
        return {"y": lax.rem(y + OFFSETS[place], LINE)}

    def at_z(place):
        return {"z": lax.rem(z + OFFSETS[place], LINE)}

    partner = {"c": other}

    load_values = pltpu.make_async_copy(expression, values_in, loaded.at[0])
    load_labels = pltpu.make_async_copy(labels, labels_in, loaded.at[1])
    load_values.start()
    load_labels.start()
    barrier = pltpu.get_barrier_semaphore()
    peers = [partner]
    for place in range(1, LINE):
        peers += [at_x(place), at_x(place, other), at_y(place), at_z(place)]
    for peer in peers:
        pl.semaphore_signal(barrier, inc=1, device_id=peer, device_id_type=pl.DeviceIdType.MESH)

    def remote(src, dst, send_sem, recv_sem, device):
        return pltpu.make_async_remote_copy(
            src_ref=src, dst_ref=dst, send_sem=send_sem, recv_sem=recv_sem,
            device_id=device, device_id_type=pl.DeviceIdType.MESH,
        )

    started = []

    def send(*args):
        copy = remote(*args)
        copy.start()
        started.append(copy)

    sample = lax.broadcasted_iota(jnp.int32, (SAMPLES, SAMPLES), 0)
    hits = jnp.where(sample == resample[...], 1.0, 0.0).astype(bf16)
    times = lax.dot_general(
        jnp.ones((16, SAMPLES), bf16), hits, NT, preferred_element_type=f32
    )
    present = jnp.where(times > 0.5, 1.0, 0.0)
    if compact:
        before = jnp.where(
            sample < lax.broadcasted_iota(jnp.int32, (SAMPLES, SAMPLES), 1), 1.0, 0.0
        ).astype(bf16)
        rank = jnp.dot(present.astype(bf16), before, preferred_element_type=f32)
        place_of = jnp.where(present > 0.5, rank, -1.0)[0:1, :].astype(jnp.int32)
    else:
        place_of = lax.broadcasted_iota(jnp.int32, (1, SAMPLES), 1)
    count_out[0] = jnp.sum(present[0:1, :].astype(jnp.int32))
    times = times[0:1, :]
    pick = jnp.where(
        lax.broadcasted_iota(jnp.int32, (depth, SAMPLES), 0) == place_of, 1.0, 0.0
    ).astype(bf16)
    load_values.wait()
    values = values_in[...]
    mean = jnp.sum(values * times, axis=1, keepdims=True) * (1.0 / SAMPLES)
    centered = values - mean
    total = jnp.sum(centered * centered * times, axis=1, keepdims=True)
    scaled = (centered * lax.rsqrt(total + 1e-06)).astype(bf16)
    weighted = (scaled.astype(f32) * times).astype(bf16)
    side = lax.dot_general(weighted, pick, NT, preferred_element_type=f32)
    front = lax.dot_general(scaled, pick, NT, preferred_element_type=f32)
    load_labels.wait()
    marks = labels_in[...].astype(f32)
    module = lax.broadcasted_iota(jnp.int32, (K, depth), 0).astype(f32) - 150.0
    module = jnp.where(lax.broadcasted_iota(jnp.int32, (K, depth), 1) == depth - 1, module, 0.0)
    front = front + lax.dot_general(
        marks.astype(bf16), module.astype(bf16), (((0,), (0,)), ((), ())),
        preferred_element_type=f32,
    )
    front = front.astype(bf16)
    rows[pl.ds(pl.multiple_of(core * OWN, OWN), OWN), :] = side.astype(bf16)
    cols[0:HALF, :] = front[0:HALF]
    cols[EARLY // 2 : EARLY // 2 + HALF, :] = front[HALF:OWN]
    place_xc = x * 2 + core
    module = lax.broadcasted_iota(jnp.int32, (K, OWN), 0).astype(f32) - 150.0
    info[place_xc, 0:1, :] = jnp.full((1, KEEP), -1000.0, f32)
    info[place_xc, 1:2, :] = jnp.zeros((1, KEEP), f32)
    info[place_xc, 0:1, 0:OWN] = jnp.sum(marks * module, axis=0, keepdims=True)
    info[place_xc, 1:2, 0:OWN] = ref_kim[...]

    pl.semaphore_wait(barrier, len(peers))

    def row_block(chunk, c):
        return rows.at[pl.ds(pl.multiple_of(chunk * CHUNK + c * OWN, OWN), OWN), :]

    def col_block(step, part, slot):
        if step == LINE - 1:
            at = LINE * EARLY + part * (LATE // 2) + slot * HALF
        elif slot == LINE - 1:
            at = (LINE - 1) * EARLY + step * OWN + part * HALF
        else:
            at = step * EARLY + part * (EARLY // 2) + slot * HALF
        return cols.at[pl.ds(at, HALF), :]

    def near_index(part, place):
        return part * LINE + place

    def far_index(part, step, slot):
        return (part * LINE + step) * LINE + slot

    along = (at_z, at_y)
    across = (at_y, at_z)

    def group(place, flip):
        if place == 0:
            return partner
        return at_x(place) if flip == 0 else at_x(place, other)

    mates = [(0, 1)] + [(place, flip) for place in range(1, LINE) for flip in range(2)]

    def to_mates(buffer, send_sem, recv_sem):
        for place, flip in mates:
            send(
                buffer.at[place_xc], buffer.at[place_xc], send_sem.at[place * 2 + flip],
                recv_sem.at[SEEN_AS[place] * 2 + flip], group(place, flip),
            )

    def from_mates(buffer, send_sem, recv_sem):
        for place, flip in mates:
            there = lax.rem(x + OFFSETS[place], LINE) * 2 + (core if flip == 0 else other)
            remote(
                buffer.at[there], buffer.at[there], send_sem.at[place * 2 + flip],
                recv_sem.at[place * 2 + flip], group(place, flip),
            ).wait_recv()

    def far_copy(part, slot, place):
        return remote(
            col_block(0, part, slot), col_block(SEEN_AS[place], part, slot),
            send_far.at[far_index(part, place, slot)],
            recv_far.at[far_index(part, SEEN_AS[place], slot)], across[part](place),
        )

    def forward_columns(part, slot, places):
        for place in places:
            far_copy(part, slot, place).start()

    def send_near_columns(place):
        for part in range(2):
            send(
                col_block(0, part, 0), col_block(0, part, SEEN_AS[place]),
                send_near.at[near_index(part, place)],
                recv_near.at[near_index(part, SEEN_AS[place])], along[part](place),
            )

    def send_rows_to(place):
        send(
            row_block(0, core), row_block(SEEN_AS[place], core),
            send_rows.at[place], recv_rows.at[SEEN_AS[place]], at_x(place),
        )

    def own_rows():
        send(row_block(0, core), row_block(0, core), send_fwd.at[0], recv_fwd.at[0], partner)

    send_near_columns(1)
    send_near_columns(2)
    own_rows()
    to_mates(info, send_info, recv_info)
    def wait_near(part, place):
        block = col_block(0, part, place)
        remote(
            block, block, send_near.at[near_index(part, place)],
            recv_near.at[near_index(part, place)], along[part](place),
        ).wait_recv()

    def wait_far(step, slots):
        for part in range(2):
            for slot in slots:
                block = col_block(step, part, slot)
                remote(
                    block, block, send_far.at[far_index(part, step, slot)],
                    recv_far.at[far_index(part, step, slot)], across[part](step),
                ).wait_recv()

    def pass_rows(chunk):
        block = row_block(chunk, core)
        remote(block, block, send_rows.at[chunk], recv_rows.at[chunk], at_x(chunk)).wait_recv()
        copy = remote(block, block, send_fwd.at[chunk], recv_fwd.at[chunk], partner)
        copy.start()

    def wait_rows(chunk):
        block = row_block(chunk, other)
        remote(block, block, send_fwd.at[chunk], recv_fwd.at[chunk], partner).wait_recv()

    for part in range(2):
        forward_columns(part, 0, (1, 2))
    send_rows_to(1)
    send_rows_to(2)
    send_rows_to(3)

    acc[...] = jnp.zeros_like(acc)
    for place in range(1, LINE - 1):
        for part in range(2):
            wait_near(part, place)
            forward_columns(part, place, (1, 2))
    send_near_columns(LINE - 1)
    for slot in range(LINE - 1):
        for part in range(2):
            forward_columns(part, slot, (LINE - 1,))
    wait_rows(0)

    def take_info():
        from_mates(info, send_info, recv_info)
        which = lax.broadcasted_iota(jnp.int32, (KP, KEEP), 0).astype(f32) - 150.0
        for index in range(2 * LINE):
            side_lt[:, index * KEEP : (index + 1) * KEEP] = jnp.where(
                which == info[index, 0:1, :], 1.0, 0.0
            ).astype(bf16)
        blank = jnp.zeros((1, CHUNK - KEEP), f32)
        for chunk in range(LINE):
            there = lax.rem(x + OFFSETS[chunk], LINE) * 2
            first = jnp.concatenate([info[there, 0:1, :] + 1000.0, blank], axis=1)
            second = jnp.concatenate([info[there + 1, 0:1, :] + 1000.0, blank], axis=1)
            both = first + pltpu.roll(second, OWN, 1) - 1000.0
            side_ids[0:1, chunk * CHUNK : (chunk + 1) * CHUNK] = both

    def pair_slice(chunk, c):
        return acc.at[:, pl.ds(pl.multiple_of(chunk * CHUNK + c * 256, 128), KEEP)]

    def to_partner(chunk):
        return remote(
            pair_slice(chunk, other), pair.at[chunk], send_pair.at[chunk], recv_pair.at[chunk],
            partner,
        )

    def to_owner(chunk):
        return remote(
            sent.at[chunk], got.at[SEEN_AS[chunk]], send_sum.at[chunk],
            recv_sum.at[SEEN_AS[chunk]], at_x(chunk),
        )

    def pass_sum(chunk):
        to_partner(chunk).wait_recv()
        mine = acc[:, pl.ds(pl.multiple_of(chunk * CHUNK + core * 256, 128), KEEP)]
        sent[chunk] = (mine + pair[chunk]).astype(bf16)
        to_owner(chunk).start()

    def make_labels(base, width):
        last = lax.broadcasted_iota(jnp.int32, (16, depth), 1) == depth - 1
        ids = lax.dot_general(
            jnp.where(last, 1.0, 0.0).astype(bf16), cols[pl.ds(base, width), :], NT,
            preferred_element_type=f32,
        )
        which = lax.broadcasted_iota(jnp.int32, (KP, width), 0).astype(f32) - 150.0
        return jnp.where(which == ids[0:1, :], 1.0, 0.0).astype(bf16)

    def score(into, base, width, side_at):
        side_block = rows[pl.ds(side_at, TILE), :]
        for start in range(0, width, 256):
            size = min(256, width - start)
            scores = lax.dot_general(
                cols[pl.ds(base + start, size), :], side_block, NT, preferred_element_type=f32
            )
            squares = scores * scores
            into[start : start + size, :] = (squares * squares * squares).astype(bf16)

    def count(held, width, side_at, module_rows):
        acc[:, pl.ds(side_at, TILE)] += jnp.dot(
            module_rows, held[0:width, :], preferred_element_type=f32
        )

    soon = (LINE - 1) * 3
    later = soon + (LINE - 1) * 2

    def task(t):
        group = jnp.where(
            t < soon, t // 3, jnp.where(t < later, (t - soon) // 2, LINE - 1)
        )
        tile = jnp.where(
            t < soon, lax.rem(t, 3), jnp.where(t < later, 3 + lax.rem(t + 1, 2), t - later)
        )
        return group, pl.multiple_of(group * EARLY, HALF), pl.multiple_of(tile * TILE, TILE)

    def score_task(into, t):
        group, base, side_at = task(t)
        score(into, base, EARLY, side_at)

    def count_task(held, t):
        group, base, side_at = task(t)
        count(held, EARLY, side_at, lt[group])

    lt[0] = make_labels(0, EARLY)
    score_task(even, 0)
    pass_rows(1)
    pass_rows(2)
    take_info()

    def two_tiles(u, carry):
        @pl.when(u == 0)
        def _():
            wait_rows(1)
            wait_rows(2)

        for far in range(1, LINE - 1):

            @pl.when(u == far)
            def _():
                wait_far(far, range(LINE - 1))
                lt[far] = make_labels(far * EARLY, EARLY)
                if far == LINE - 2:
                    for part in range(2):
                        wait_near(part, LINE - 1)
                        forward_columns(part, LINE - 1, (1, 2, 3))
                    pass_rows(3)

        @pl.when(u == (soon - 1) // 2)
        def _():
            wait_rows(3)

        @pl.when(u == (later - 1) // 2)
        def _():
            wait_far(1, (LINE - 1,))
            wait_far(2, (LINE - 1,))
            lt[LINE - 1] = make_labels((LINE - 1) * EARLY, EARLY)

        count_task(even, 2 * u)
        score_task(odd, 2 * u + 1)
        count_task(odd, 2 * u + 1)
        score_task(even, 2 * u + 2)
        return carry

    pairs = (later + TILES - 2) // 2
    lax.fori_loop(0, pairs, two_tiles, 0)
    count_task(even, 2 * pairs)
    score_task(odd, 2 * pairs + 1)
    wait_far(LINE - 1, range(LINE))
    lt_late[...] = make_labels(LINE * EARLY, LATE)
    count_task(odd, 2 * pairs + 1)
    score(even, LINE * EARLY, LATE, (TILES - 1) * TILE)
    for turn in range(TILES):
        side_at = (TILES - 1 - turn) * TILE
        held, into = (even, odd) if turn % 2 == 0 else (odd, even)
        count(held, LATE, side_at, lt_late[...])
        if turn < TILES - 1:
            score(into, LINE * EARLY, LATE, side_at - TILE)
        which = lax.broadcasted_iota(jnp.int32, (KP, TILE), 0).astype(f32) - 150.0
        done = acc[:, side_at : side_at + TILE]
        hit = which == side_ids[0:1, side_at : side_at + TILE]
        kim_rows[0:1, side_at : side_at + TILE] = jnp.sum(
            jnp.where(hit, done, 0.0), axis=0, keepdims=True
        )
        kim_rows[1:2, side_at : side_at + TILE] = jnp.sum(done, axis=0, keepdims=True)
        if turn > 0:
            to_partner(LINE - turn).start()

    for chunk in range(LINE):
        there = lax.rem(x + OFFSETS[chunk], LINE) * 2
        for c in range(2):
            for kind in range(2):
                piece = kim_rows[kind : kind + 1, chunk * CHUNK + c * 256 : chunk * CHUNK + c * 256 + KEEP]
                if c == 1:
                    piece = pltpu.roll(piece, KEEP - 64, 1)
                parts[place_xc, kind, pl.ds(there + c, 1), :] = piece
    to_mates(parts, send_part, recv_part)
    for chunk in range(LINE - 1, 0, -1):
        pass_sum(chunk)

    from_mates(parts, send_part, recv_part)
    kim, rowsum = parts[0, 0], parts[0, 1]
    for index in range(1, 2 * LINE):
        kim = kim + parts[index, 0]
        rowsum = rowsum + parts[index, 1]
    for index in range(2 * LINE):
        at = slice(index * KEEP, (index + 1) * KEEP)
        k, r, ref = kim[index : index + 1], rowsum[index : index + 1], info[index, 1:2, :]
        one, none = jnp.ones_like(k), jnp.zeros_like(k)
        stats[:, at] = jnp.concatenate([k, k * k, ref, ref * ref, k * ref, r, one, none], axis=0)
    exact = stats[...]
    high = exact.astype(bf16).astype(f32)
    middle = (exact - high).astype(bf16).astype(f32)
    low = exact - high - middle
    split = jnp.concatenate([high, middle, low, jnp.zeros_like(low)], axis=0).astype(bf16)
    sums = lax.dot_general(split, side_lt[...], NT, preferred_element_type=f32)
    total_sums = sums[0:8] + sums[8:16] + sums[16:24]

    def wait_sent(copies):
        for copy in copies:
            copy.wait_send()

    for axis, (mine, buffer, at) in enumerate(((y, sums_y, at_y), (z, sums_z, at_z))):
        buffer[mine] = total_sums
        copies = []
        for place in range(1, LINE):
            copy = remote(
                buffer.at[mine], buffer.at[mine], send_yz.at[axis * LINE + place],
                recv_yz.at[axis * LINE + SEEN_AS[place]], at(place),
            )
            copy.start()
            copies.append(copy)
        for place in range(1, LINE):
            there = lax.rem(mine + OFFSETS[place], LINE)
            remote(
                buffer.at[there], buffer.at[there], send_yz.at[axis * LINE + place],
                recv_yz.at[axis * LINE + place], at(place),
            ).wait_recv()
        total_sums = buffer[0]
        for index in range(1, LINE):
            total_sums = total_sums + buffer[index]
        wait_sent(copies)

    s_k, s_kk, s_y, s_yy, s_ky, s_r, n = (total_sums[i : i + 1, 0:K] for i in range(7))
    mean_x = s_k / (n * n)
    var_x = jnp.maximum(s_kk / (n * n * n) - mean_x * mean_x, 0.0001)
    mean_y = s_y / n
    var_y = jnp.maximum(s_yy / n - mean_y * mean_y, 0.01)
    cross = s_ky / (n * n) - mean_x * mean_y
    between = (s_r - s_k) / (n * (float(G) - n))
    pres_out[0:1, :] = (mean_x - between) * jnp.sqrt(n / var_x)
    pres_out[1:2, :] = cross * jnp.sqrt(n / (var_x * var_y))

    to_partner(0).wait_recv()
    conn = acc[:, pl.ds(pl.multiple_of(core * 256, 128), KEEP)] + pair[0]
    for chunk in range(1, LINE):
        remote(
            sent.at[chunk], got.at[chunk], send_sum.at[chunk], recv_sum.at[chunk], at_x(chunk)
        ).wait_recv()
        conn = conn + got[chunk].astype(f32)
    conn = jnp.where(core == 0, conn, pltpu.roll(conn, KEEP - 64, 1))
    conn_out[...] = conn[0:K, 0:OWN]

    wait_sent(started)
    for place in range(1, LINE):
        for part in range(2):
            for slot in range(LINE):
                far_copy(part, slot, place).wait_send()
    for chunk in range(1, LINE):
        block = row_block(chunk, core)
        remote(block, block, send_fwd.at[chunk], recv_fwd.at[chunk], partner).wait_send()
        to_owner(chunk).wait_send()
    for chunk in range(LINE):
        to_partner(chunk).wait_send()


def whole(depth, compact, collective, resample, expression, labels, ref_kim):
    f32, bf16 = jnp.float32, jnp.bfloat16
    dma = pltpu.SemaphoreType.DMA
    vmem, hbm = pl.BlockSpec(memory_space=pltpu.VMEM), pl.BlockSpec(memory_space=pl.ANY)
    scratch = [
        pltpu.VMEM((OWN, SAMPLES), f32),
        pltpu.VMEM((K, OWN), jnp.int32),
        pltpu.VMEM((ROWS, depth), bf16),
        pltpu.VMEM((COLS, depth), bf16),
        pltpu.VMEM((LINE, KP, EARLY), bf16),
        pltpu.VMEM((KP, LATE), bf16),
        pltpu.VMEM((LATE, TILE), bf16),
        pltpu.VMEM((LATE, TILE), bf16),
        pltpu.VMEM((KP, ROWS), f32),
        pltpu.VMEM((LINE, KP, KEEP), f32),
        pltpu.VMEM((LINE, KP, KEEP), bf16),
        pltpu.VMEM((LINE, KP, KEEP), bf16),
        pltpu.VMEM((2 * LINE, 2, KEEP), f32),
        pltpu.VMEM((8, ROWS), f32),
        pltpu.VMEM((KP, 2 * LINE * KEEP), bf16),
        pltpu.VMEM((8, ROWS), f32),
        pltpu.VMEM((2 * LINE, 2, 2 * LINE, KEEP), f32),
        pltpu.VMEM((8, 2 * LINE * KEEP), f32),
        pltpu.VMEM((LINE, 8, KP), f32),
        pltpu.VMEM((LINE, 8, KP), f32),
        dma((2,)),
    ]
    for count in (
        LINE, LINE, 2 * LINE, 2 * LINE * LINE, LINE, LINE, 2 * LINE, 2 * LINE, 2 * LINE,
    ):
        scratch += [dma((count,)), dma((count,))]
    return pl.pallas_call(
        functools.partial(kernel, depth, compact),
        out_shape=(
            jax.ShapeDtypeStruct((K, OWN), f32),
            jax.ShapeDtypeStruct((2, K), f32),
            jax.ShapeDtypeStruct((1,), jnp.int32),
        ),
        in_specs=[vmem, hbm, hbm, vmem],
        out_specs=(vmem, vmem, pl.BlockSpec(memory_space=pltpu.SMEM)),
        scratch_shapes=scratch,
        compiler_params=pltpu.CompilerParams(
            collective_id=collective, has_side_effects=True, vmem_limit_bytes=60 * 1024 * 1024
        ),
        name=f"network_{depth}",
    )(resample, expression, labels, ref_kim)


def local(expression, resample, labels, ref_kim):
    operands = (
        resample.reshape(1, SAMPLES), expression.T, labels.T, ref_kim.reshape(1, OWN),
    )
    conn, preservation, distinct = whole(256, True, 0, *operands)
    conn, preservation = lax.cond(
        distinct[0] <= 255,
        lambda *ready: ready[:2],
        lambda *ready: whole(512, False, 1, *ready[2:])[:2],
        conn, preservation, *operands,
    )
    return conn.T, preservation


def solution(mesh):
    torus = Mesh(mesh.devices.reshape(4, 4, 2, 2, 2), AXES)
    placed = (P(None, AXES), P(), P(AXES, None), P(AXES))
    return jax.shard_map(
        local, mesh=torus, in_specs=placed, out_specs=(P(AXES, None), P()), check_vma=False
    )
```

```python
import functools

import jax
import jax.numpy as jnp
from jax import lax
from jax.experimental import pallas as pl
from jax.experimental.pallas import tpu as pltpu
from jax.sharding import Mesh
from jax.sharding import PartitionSpec as P

G = 40960
SAMPLES = 384
K = 300
KP = 304
OWN = 320
HALF = OWN // 2
LINE = 4
CHUNK = 2 * OWN
EARLY = 2 * (LINE - 1) * HALF
LATE = 2 * LINE * HALF
ROWS = LINE * CHUNK
COLS = LINE * EARLY + LATE
TILE = 512
TILES = ROWS // TILE
KEEP = 384
AXES = ("z", "y", "xh", "c", "xl")
OFFSETS = (0, 1, 3, 2)
SEEN_AS = (0, 2, 1, 3)
NT = (((1,), (1,)), ((), ()))


def kernel(
    depth, compact, resample, expression, labels, ref_kim, conn_out, pres_out, count_out,
    values_in, labels_in, rows, cols, lt, lt_late, even, odd, acc, pair, sent, got, sent_shared, got_shared, info, side_ids, side_lt,
    kim_rows, parts, stats, sums_y, sums_z, loaded,
    send_rows, recv_rows, send_fwd, recv_fwd, send_near, recv_near, send_far, recv_far,
    send_pair, recv_pair, send_sum, recv_sum, send_info, recv_info, send_part, recv_part,
    send_yz, recv_yz,
):
    f32, bf16 = jnp.float32, jnp.bfloat16
    z, y, core = lax.axis_index("z"), lax.axis_index("y"), lax.axis_index("c")
    x = lax.axis_index("xh") * 2 + lax.axis_index("xl")
    other = 1 - core

    def at_x(place, c=None):
        there = lax.rem(x + OFFSETS[place], LINE)
        device = {"xh": there // 2, "xl": lax.rem(there, 2)}
        if c is not None:
            device["c"] = c
        return device

    def at_y(place):
        return {"y": lax.rem(y + OFFSETS[place], LINE)}

    def at_z(place):
        return {"z": lax.rem(z + OFFSETS[place], LINE)}

    partner = {"c": other}

    load_values = pltpu.make_async_copy(expression, values_in, loaded.at[0])
    load_labels = pltpu.make_async_copy(labels, labels_in, loaded.at[1])
    load_values.start()
    load_labels.start()
    barrier = pltpu.get_barrier_semaphore()
    peers = [partner]
    for place in range(1, LINE):
        peers += [at_x(place), at_x(place, other), at_y(place), at_z(place)]
    for peer in peers:
        pl.semaphore_signal(barrier, inc=1, device_id=peer, device_id_type=pl.DeviceIdType.MESH)

    def remote(src, dst, send_sem, recv_sem, device):
        return pltpu.make_async_remote_copy(
            src_ref=src, dst_ref=dst, send_sem=send_sem, recv_sem=recv_sem,
            device_id=device, device_id_type=pl.DeviceIdType.MESH,
        )

    started = []

    def send(*args):
        copy = remote(*args)
        copy.start()
        started.append(copy)

    sample = lax.broadcasted_iota(jnp.int32, (SAMPLES, SAMPLES), 0)
    hits = jnp.where(sample == resample[...], 1.0, 0.0).astype(bf16)
    times = lax.dot_general(
        jnp.ones((16, SAMPLES), bf16), hits, NT, preferred_element_type=f32
    )
    present = jnp.where(times > 0.5, 1.0, 0.0)
    if compact:
        before = jnp.where(
            sample < lax.broadcasted_iota(jnp.int32, (SAMPLES, SAMPLES), 1), 1.0, 0.0
        ).astype(bf16)
        rank = jnp.dot(present.astype(bf16), before, preferred_element_type=f32)
        place_of = jnp.where(present > 0.5, rank, -1.0)[0:1, :].astype(jnp.int32)
    else:
        place_of = lax.broadcasted_iota(jnp.int32, (1, SAMPLES), 1)
    count_out[0] = jnp.sum(present[0:1, :].astype(jnp.int32))
    times = times[0:1, :]
    pick = jnp.where(
        lax.broadcasted_iota(jnp.int32, (depth, SAMPLES), 0) == place_of, 1.0, 0.0
    ).astype(bf16)
    load_values.wait()
    values = values_in[...]
    mean = jnp.sum(values * times, axis=1, keepdims=True) * (1.0 / SAMPLES)
    centered = values - mean
    total = jnp.sum(centered * centered * times, axis=1, keepdims=True)
    scaled = (centered * lax.rsqrt(total + 1e-06)).astype(bf16)
    weighted = (scaled.astype(f32) * times).astype(bf16)
    side = lax.dot_general(weighted, pick, NT, preferred_element_type=f32)
    front = lax.dot_general(scaled, pick, NT, preferred_element_type=f32)
    load_labels.wait()
    marks = labels_in[...].astype(f32)
    module = lax.broadcasted_iota(jnp.int32, (K, depth), 0).astype(f32) - 150.0
    module = jnp.where(lax.broadcasted_iota(jnp.int32, (K, depth), 1) == depth - 1, module, 0.0)
    front = front + lax.dot_general(
        marks.astype(bf16), module.astype(bf16), (((0,), (0,)), ((), ())),
        preferred_element_type=f32,
    )
    front = front.astype(bf16)
    rows[pl.ds(pl.multiple_of(core * OWN, OWN), OWN), :] = side.astype(bf16)
    cols[0:HALF, :] = front[0:HALF]
    cols[EARLY // 2 : EARLY // 2 + HALF, :] = front[HALF:OWN]
    place_xc = x * 2 + core
    module = lax.broadcasted_iota(jnp.int32, (K, OWN), 0).astype(f32) - 150.0
    info[place_xc, 0:1, :] = jnp.full((1, KEEP), -1000.0, f32)
    info[place_xc, 1:2, :] = jnp.zeros((1, KEEP), f32)
    info[place_xc, 0:1, 0:OWN] = jnp.sum(marks * module, axis=0, keepdims=True)
    info[place_xc, 1:2, 0:OWN] = ref_kim[...]

    pl.semaphore_wait(barrier, len(peers))

    def row_block(chunk, c):
        return rows.at[pl.ds(pl.multiple_of(chunk * CHUNK + c * OWN, OWN), OWN), :]

    def col_block(step, part, slot):
        if step == LINE - 1:
            at = LINE * EARLY + part * (LATE // 2) + slot * HALF
        elif slot == LINE - 1:
            at = (LINE - 1) * EARLY + step * OWN + part * HALF
        else:
            at = step * EARLY + part * (EARLY // 2) + slot * HALF
        return cols.at[pl.ds(at, HALF), :]

    def near_index(part, place):
        return part * LINE + place

    def far_index(part, step, slot):
        return (part * LINE + step) * LINE + slot

    along = (at_z, at_y)
    across = (at_y, at_z)

    def group(place, flip):
        if place == 0:
            return partner
        return at_x(place) if flip == 0 else at_x(place, other)

    mates = [(0, 1)] + [(place, flip) for place in range(1, LINE) for flip in range(2)]

    def to_mates(buffer, send_sem, recv_sem):
        for place, flip in mates:
            send(
                buffer.at[place_xc], buffer.at[place_xc], send_sem.at[place * 2 + flip],
                recv_sem.at[SEEN_AS[place] * 2 + flip], group(place, flip),
            )

    def from_mates(buffer, send_sem, recv_sem):
        for place, flip in mates:
            there = lax.rem(x + OFFSETS[place], LINE) * 2 + (core if flip == 0 else other)
            remote(
                buffer.at[there], buffer.at[there], send_sem.at[place * 2 + flip],
                recv_sem.at[place * 2 + flip], group(place, flip),
            ).wait_recv()

    def far_copy(part, slot, place):
        return remote(
            col_block(0, part, slot), col_block(SEEN_AS[place], part, slot),
            send_far.at[far_index(part, place, slot)],
            recv_far.at[far_index(part, SEEN_AS[place], slot)], across[part](place),
        )

    def forward_columns(part, slot, places):
        for place in places:
            far_copy(part, slot, place).start()

    def send_near_columns(place):
        for part in range(2):
            send(
                col_block(0, part, 0), col_block(0, part, SEEN_AS[place]),
                send_near.at[near_index(part, place)],
                recv_near.at[near_index(part, SEEN_AS[place])], along[part](place),
            )

    def send_rows_to(place):
        send(
            row_block(0, core), row_block(SEEN_AS[place], core),
            send_rows.at[place], recv_rows.at[SEEN_AS[place]], at_x(place),
        )

    def own_rows():
        send(row_block(0, core), row_block(0, core), send_fwd.at[0], recv_fwd.at[0], partner)

    send_near_columns(1)
    send_near_columns(2)
    own_rows()
    to_mates(info, send_info, recv_info)
    def wait_near(part, place):
        block = col_block(0, part, place)
        remote(
            block, block, send_near.at[near_index(part, place)],
            recv_near.at[near_index(part, place)], along[part](place),
        ).wait_recv()

    def wait_far(step, slots):
        for part in range(2):
            for slot in slots:
                block = col_block(step, part, slot)
                remote(
                    block, block, send_far.at[far_index(part, step, slot)],
                    recv_far.at[far_index(part, step, slot)], across[part](step),
                ).wait_recv()

    def pass_rows(chunk):
        block = row_block(chunk, core)
        remote(block, block, send_rows.at[chunk], recv_rows.at[chunk], at_x(chunk)).wait_recv()
        copy = remote(block, block, send_fwd.at[chunk], recv_fwd.at[chunk], partner)
        copy.start()

    def wait_rows(chunk):
        block = row_block(chunk, other)
        remote(block, block, send_fwd.at[chunk], recv_fwd.at[chunk], partner).wait_recv()

    for part in range(2):
        forward_columns(part, 0, (1, 2))
    send_rows_to(1)
    send_rows_to(2)
    send_rows_to(3)

    acc[...] = jnp.zeros_like(acc)
    for place in range(1, LINE - 1):
        for part in range(2):
            wait_near(part, place)
            forward_columns(part, place, (1, 2))
    send_near_columns(LINE - 1)
    for slot in range(LINE - 1):
        for part in range(2):
            forward_columns(part, slot, (LINE - 1,))
    wait_rows(0)

    def take_info():
        from_mates(info, send_info, recv_info)
        which = lax.broadcasted_iota(jnp.int32, (KP, KEEP), 0).astype(f32) - 150.0
        for index in range(2 * LINE):
            side_lt[:, index * KEEP : (index + 1) * KEEP] = jnp.where(
                which == info[index, 0:1, :], 1.0, 0.0
            ).astype(bf16)
        blank = jnp.zeros((1, CHUNK - KEEP), f32)
        for chunk in range(LINE):
            there = lax.rem(x + OFFSETS[chunk], LINE) * 2
            first = jnp.concatenate([info[there, 0:1, :] + 1000.0, blank], axis=1)
            second = jnp.concatenate([info[there + 1, 0:1, :] + 1000.0, blank], axis=1)
            both = first + pltpu.roll(second, OWN, 1) - 1000.0
            side_ids[0:1, chunk * CHUNK : (chunk + 1) * CHUNK] = both

    def pair_slice(chunk, c):
        return acc.at[:, pl.ds(pl.multiple_of(chunk * CHUNK + c * 256, 128), KEEP)]

    def to_partner(chunk):
        return remote(
            pair_slice(chunk, other), pair.at[chunk], send_pair.at[chunk], recv_pair.at[chunk],
            partner,
        )

    ours = (lax.broadcasted_iota(jnp.int32, (KP // 2, 128), 1) < 64) == (core == 0)

    def summed(chunk):
        whole_at = pl.multiple_of(chunk * CHUNK + core * 384, 128)
        main = acc[:, pl.ds(whole_at, 256)]
        main = main + pair[chunk, :, pl.ds(pl.multiple_of(core * 128, 128), 256)]
        shared = acc[:, chunk * CHUNK + 256 : chunk * CHUNK + 384]
        shared = shared + pair[chunk, :, pl.ds(pl.multiple_of((1 - core) * 256, 128), 128)]
        return main, shared

    def to_owner(chunk):
        return [
            remote(
                src.at[chunk], dst.at[SEEN_AS[chunk]], send_sum.at[first + chunk],
                recv_sum.at[first + SEEN_AS[chunk]], at_x(chunk),
            )
            for src, dst, first in ((sent, got, 0), (sent_shared, got_shared, LINE))
        ]

    def pass_sum(chunk):
        to_partner(chunk).wait_recv()
        main, shared = summed(chunk)
        sent[chunk] = main.astype(bf16)
        upper = pltpu.roll(shared[KP // 2 : KP], 64, 1)
        sent_shared[chunk] = jnp.where(ours, shared[0 : KP // 2], upper).astype(bf16)
        for copy in to_owner(chunk):
            copy.start()

    def make_labels(base, width):
        last = lax.broadcasted_iota(jnp.int32, (16, depth), 1) == depth - 1
        ids = lax.dot_general(
            jnp.where(last, 1.0, 0.0).astype(bf16), cols[pl.ds(base, width), :], NT,
            preferred_element_type=f32,
        )
        which = lax.broadcasted_iota(jnp.int32, (KP, width), 0).astype(f32) - 150.0
        return jnp.where(which == ids[0:1, :], 1.0, 0.0).astype(bf16)

    def score(into, base, width, side_at):
        side_block = rows[pl.ds(side_at, TILE), :]
        for start in range(0, width, 256):
            size = min(256, width - start)
            scores = lax.dot_general(
                cols[pl.ds(base + start, size), :], side_block, NT, preferred_element_type=f32
            )
            squares = scores * scores
            into[start : start + size, :] = (squares * squares * squares).astype(bf16)

    def count(held, width, side_at, module_rows):
        acc[:, pl.ds(side_at, TILE)] += jnp.dot(
            module_rows, held[0:width, :], preferred_element_type=f32
        )

    soon = (LINE - 1) * 3
    later = soon + (LINE - 1) * 2

    def task(t):
        group = jnp.where(
            t < soon, t // 3, jnp.where(t < later, (t - soon) // 2, LINE - 1)
        )
        tile = jnp.where(
            t < soon, lax.rem(t, 3), jnp.where(t < later, 3 + lax.rem(t + 1, 2), t - later)
        )
        return group, pl.multiple_of(group * EARLY, HALF), pl.multiple_of(tile * TILE, TILE)

    def score_task(into, t):
        group, base, side_at = task(t)
        score(into, base, EARLY, side_at)

    def count_task(held, t):
        group, base, side_at = task(t)
        count(held, EARLY, side_at, lt[group])

    lt[0] = make_labels(0, EARLY)
    score_task(even, 0)
    pass_rows(1)
    pass_rows(2)
    take_info()

    def two_tiles(u, carry):
        @pl.when(u == 0)
        def _():
            wait_rows(1)
            wait_rows(2)

        for far in range(1, LINE - 1):

            @pl.when(u == far)
            def _():
                wait_far(far, range(LINE - 1))
                lt[far] = make_labels(far * EARLY, EARLY)
                if far == LINE - 2:
                    for part in range(2):
                        wait_near(part, LINE - 1)
                        forward_columns(part, LINE - 1, (1, 2, 3))
                    pass_rows(3)

        @pl.when(u == (soon - 1) // 2)
        def _():
            wait_rows(3)

        @pl.when(u == (later - 1) // 2)
        def _():
            wait_far(1, (LINE - 1,))
            wait_far(2, (LINE - 1,))
            lt[LINE - 1] = make_labels((LINE - 1) * EARLY, EARLY)

        count_task(even, 2 * u)
        score_task(odd, 2 * u + 1)
        count_task(odd, 2 * u + 1)
        score_task(even, 2 * u + 2)
        return carry

    pairs = (later + TILES - 2) // 2
    lax.fori_loop(0, pairs, two_tiles, 0)
    count_task(even, 2 * pairs)
    score_task(odd, 2 * pairs + 1)
    wait_far(LINE - 1, range(LINE))
    lt_late[...] = make_labels(LINE * EARLY, LATE)
    count_task(odd, 2 * pairs + 1)
    score(even, LINE * EARLY, LATE, (TILES - 1) * TILE)
    for turn in range(TILES):
        side_at = (TILES - 1 - turn) * TILE
        held, into = (even, odd) if turn % 2 == 0 else (odd, even)
        count(held, LATE, side_at, lt_late[...])
        if turn < TILES - 1:
            score(into, LINE * EARLY, LATE, side_at - TILE)
        which = lax.broadcasted_iota(jnp.int32, (KP, TILE), 0).astype(f32) - 150.0
        done = acc[:, side_at : side_at + TILE]
        hit = which == side_ids[0:1, side_at : side_at + TILE]
        kim_rows[0:1, side_at : side_at + TILE] = jnp.sum(
            jnp.where(hit, done, 0.0), axis=0, keepdims=True
        )
        kim_rows[1:2, side_at : side_at + TILE] = jnp.sum(done, axis=0, keepdims=True)
        if turn > 0:
            to_partner(LINE - turn).start()

    for chunk in range(LINE):
        there = lax.rem(x + OFFSETS[chunk], LINE) * 2
        for c in range(2):
            for kind in range(2):
                piece = kim_rows[kind : kind + 1, chunk * CHUNK + c * 256 : chunk * CHUNK + c * 256 + KEEP]
                if c == 1:
                    piece = pltpu.roll(piece, KEEP - 64, 1)
                parts[place_xc, kind, pl.ds(there + c, 1), :] = piece
    to_mates(parts, send_part, recv_part)
    for chunk in range(LINE - 1, 0, -1):
        pass_sum(chunk)

    from_mates(parts, send_part, recv_part)
    kim, rowsum = parts[0, 0], parts[0, 1]
    for index in range(1, 2 * LINE):
        kim = kim + parts[index, 0]
        rowsum = rowsum + parts[index, 1]
    for index in range(2 * LINE):
        at = slice(index * KEEP, (index + 1) * KEEP)
        k, r, ref = kim[index : index + 1], rowsum[index : index + 1], info[index, 1:2, :]
        one, none = jnp.ones_like(k), jnp.zeros_like(k)
        stats[:, at] = jnp.concatenate([k, k * k, ref, ref * ref, k * ref, r, one, none], axis=0)
    exact = stats[...]
    high = exact.astype(bf16).astype(f32)
    middle = (exact - high).astype(bf16).astype(f32)
    low = exact - high - middle
    split = jnp.concatenate([high, middle, low, jnp.zeros_like(low)], axis=0).astype(bf16)
    sums = lax.dot_general(split, side_lt[...], NT, preferred_element_type=f32)
    total_sums = sums[0:8] + sums[8:16] + sums[16:24]

    def wait_sent(copies):
        for copy in copies:
            copy.wait_send()

    for axis, (mine, buffer, at) in enumerate(((y, sums_y, at_y), (z, sums_z, at_z))):
        buffer[mine] = total_sums
        copies = []
        for place in range(1, LINE):
            copy = remote(
                buffer.at[mine], buffer.at[mine], send_yz.at[axis * LINE + place],
                recv_yz.at[axis * LINE + SEEN_AS[place]], at(place),
            )
            copy.start()
            copies.append(copy)
        for place in range(1, LINE):
            there = lax.rem(mine + OFFSETS[place], LINE)
            remote(
                buffer.at[there], buffer.at[there], send_yz.at[axis * LINE + place],
                recv_yz.at[axis * LINE + place], at(place),
            ).wait_recv()
        total_sums = buffer[0]
        for index in range(1, LINE):
            total_sums = total_sums + buffer[index]
        wait_sent(copies)

    s_k, s_kk, s_y, s_yy, s_ky, s_r, n = (total_sums[i : i + 1, 0:K] for i in range(7))
    mean_x = s_k / (n * n)
    var_x = jnp.maximum(s_kk / (n * n * n) - mean_x * mean_x, 0.0001)
    mean_y = s_y / n
    var_y = jnp.maximum(s_yy / n - mean_y * mean_y, 0.01)
    cross = s_ky / (n * n) - mean_x * mean_y
    between = (s_r - s_k) / (n * (float(G) - n))
    pres_out[0:1, :] = (mean_x - between) * jnp.sqrt(n / var_x)
    pres_out[1:2, :] = cross * jnp.sqrt(n / (var_x * var_y))

    to_partner(0).wait_recv()
    main, shared = summed(0)
    for chunk in range(1, LINE):
        for src, dst, first in ((sent, got, 0), (sent_shared, got_shared, LINE)):
            remote(
                src.at[chunk], dst.at[chunk], send_sum.at[first + chunk],
                recv_sum.at[first + chunk], at_x(chunk),
            ).wait_recv()
        main = main + got[chunk].astype(f32)
        lower = got_shared[chunk].astype(f32)
        shared = shared + jnp.concatenate([lower, pltpu.roll(lower, 64, 1)], axis=0)
    conn = jnp.where(
        core == 0,
        jnp.concatenate([main, shared], axis=1),
        pltpu.roll(jnp.concatenate([shared, main], axis=1), KEEP - 64, 1),
    )
    conn_out[...] = conn[0:K, 0:OWN]

    wait_sent(started)
    for place in range(1, LINE):
        for part in range(2):
            for slot in range(LINE):
                far_copy(part, slot, place).wait_send()
    for chunk in range(1, LINE):
        block = row_block(chunk, core)
        remote(block, block, send_fwd.at[chunk], recv_fwd.at[chunk], partner).wait_send()
        for copy in to_owner(chunk):
            copy.wait_send()
    for chunk in range(LINE):
        to_partner(chunk).wait_send()


def whole(depth, compact, collective, resample, expression, labels, ref_kim):
    f32, bf16 = jnp.float32, jnp.bfloat16
    dma = pltpu.SemaphoreType.DMA
    vmem, hbm = pl.BlockSpec(memory_space=pltpu.VMEM), pl.BlockSpec(memory_space=pl.ANY)
    scratch = [
        pltpu.VMEM((OWN, SAMPLES), f32),
        pltpu.VMEM((K, OWN), jnp.int32),
        pltpu.VMEM((ROWS, depth), bf16),
        pltpu.VMEM((COLS, depth), bf16),
        pltpu.VMEM((LINE, KP, EARLY), bf16),
        pltpu.VMEM((KP, LATE), bf16),
        pltpu.VMEM((LATE, TILE), bf16),
        pltpu.VMEM((LATE, TILE), bf16),
        pltpu.VMEM((KP, ROWS), f32),
        pltpu.VMEM((LINE, KP, KEEP), f32),
        pltpu.VMEM((LINE, KP, 256), bf16),
        pltpu.VMEM((LINE, KP, 256), bf16),
        pltpu.VMEM((LINE, KP // 2, 128), bf16),
        pltpu.VMEM((LINE, KP // 2, 128), bf16),
        pltpu.VMEM((2 * LINE, 2, KEEP), f32),
        pltpu.VMEM((8, ROWS), f32),
        pltpu.VMEM((KP, 2 * LINE * KEEP), bf16),
        pltpu.VMEM((8, ROWS), f32),
        pltpu.VMEM((2 * LINE, 2, 2 * LINE, KEEP), f32),
        pltpu.VMEM((8, 2 * LINE * KEEP), f32),
        pltpu.VMEM((LINE, 8, KP), f32),
        pltpu.VMEM((LINE, 8, KP), f32),
        dma((2,)),
    ]
    for count in (
        LINE, LINE, 2 * LINE, 2 * LINE * LINE, LINE, 2 * LINE, 2 * LINE, 2 * LINE, 2 * LINE,
    ):
        scratch += [dma((count,)), dma((count,))]
    return pl.pallas_call(
        functools.partial(kernel, depth, compact),
        out_shape=(
            jax.ShapeDtypeStruct((K, OWN), f32),
            jax.ShapeDtypeStruct((2, K), f32),
            jax.ShapeDtypeStruct((1,), jnp.int32),
        ),
        in_specs=[vmem, hbm, hbm, vmem],
        out_specs=(vmem, vmem, pl.BlockSpec(memory_space=pltpu.SMEM)),
        scratch_shapes=scratch,
        compiler_params=pltpu.CompilerParams(
            collective_id=collective, has_side_effects=True, vmem_limit_bytes=60 * 1024 * 1024
        ),
        name=f"network_{depth}",
    )(resample, expression, labels, ref_kim)


def local(expression, resample, labels, ref_kim):
    operands = (
        resample.reshape(1, SAMPLES), expression.T, labels.T, ref_kim.reshape(1, OWN),
    )
    conn, preservation, distinct = whole(256, True, 0, *operands)
    conn, preservation = lax.cond(
        distinct[0] <= 255,
        lambda *ready: ready[:2],
        lambda *ready: whole(512, False, 1, *ready[2:])[:2],
        conn, preservation, *operands,
    )
    return conn.T, preservation


def solution(mesh):
    torus = Mesh(mesh.devices.reshape(4, 4, 2, 2, 2), AXES)
    placed = (P(None, AXES), P(), P(AXES, None), P(AXES))
    return jax.shard_map(
        local, mesh=torus, in_specs=placed, out_specs=(P(AXES, None), P()), check_vma=False
    )
```

```python
import functools

import jax
import jax.numpy as jnp
from jax import lax
from jax.experimental import pallas as pl
from jax.experimental.pallas import tpu as pltpu
from jax.sharding import Mesh
from jax.sharding import PartitionSpec as P

G = 40960
SAMPLES = 384
K = 300
KP = 304
OWN = 320
HALF = OWN // 2
LINE = 4
OFTEN = 8
CHUNK = 2 * OWN
EARLY = 2 * (LINE - 1) * HALF
LATE = 2 * LINE * HALF
ROWS = LINE * CHUNK
COLS = LINE * EARLY + LATE
TILE = 512
TILES = ROWS // TILE
KEEP = 384
AXES = ("z", "y", "xh", "c", "xl")
OFFSETS = (0, 1, 3, 2)
SEEN_AS = (0, 2, 1, 3)
NT = (((1,), (1,)), ((), ()))


def kernel(
    depth, compact, resample, expression, labels, ref_kim, conn_out, pres_out, count_out,
    values_in, labels_in, rows, cols, lt, lt_late, even, odd, acc, pair, sent, got, sent_shared, got_shared, info, side_ids, side_lt,
    kim_rows, parts, stats, sums_y, sums_z, loaded,
    send_rows, recv_rows, send_fwd, recv_fwd, send_near, recv_near, send_far, recv_far,
    send_pair, recv_pair, send_sum, recv_sum, send_info, recv_info, send_part, recv_part,
    send_yz, recv_yz,
):
    f32, bf16 = jnp.float32, jnp.bfloat16
    z, y, core = lax.axis_index("z"), lax.axis_index("y"), lax.axis_index("c")
    x = lax.axis_index("xh") * 2 + lax.axis_index("xl")
    other = 1 - core

    def at_x(place, c=None):
        there = lax.rem(x + OFFSETS[place], LINE)
        device = {"xh": there // 2, "xl": lax.rem(there, 2)}
        if c is not None:
            device["c"] = c
        return device

    def at_y(place):
        return {"y": lax.rem(y + OFFSETS[place], LINE)}

    def at_z(place):
        return {"z": lax.rem(z + OFFSETS[place], LINE)}

    partner = {"c": other}

    load_values = pltpu.make_async_copy(expression, values_in, loaded.at[0])
    load_labels = pltpu.make_async_copy(labels, labels_in, loaded.at[1])
    load_values.start()
    load_labels.start()
    barrier = pltpu.get_barrier_semaphore()
    peers = [partner]
    for place in range(1, LINE):
        peers += [at_x(place), at_x(place, other), at_y(place), at_z(place)]
    for peer in peers:
        pl.semaphore_signal(barrier, inc=1, device_id=peer, device_id_type=pl.DeviceIdType.MESH)

    def remote(src, dst, send_sem, recv_sem, device):
        return pltpu.make_async_remote_copy(
            src_ref=src, dst_ref=dst, send_sem=send_sem, recv_sem=recv_sem,
            device_id=device, device_id_type=pl.DeviceIdType.MESH,
        )

    started = []

    def send(*args):
        copy = remote(*args)
        copy.start()
        started.append(copy)

    sample = lax.broadcasted_iota(jnp.int32, (SAMPLES, SAMPLES), 0)
    hits = jnp.where(sample == resample[...], 1.0, 0.0).astype(bf16)
    times = lax.dot_general(
        jnp.ones((16, SAMPLES), bf16), hits, NT, preferred_element_type=f32
    )
    present = jnp.where(times > 0.5, 1.0, 0.0)
    if compact:
        before = jnp.where(
            sample < lax.broadcasted_iota(jnp.int32, (SAMPLES, SAMPLES), 1), 1.0, 0.0
        ).astype(bf16)
        rank = jnp.dot(present.astype(bf16), before, preferred_element_type=f32)
        place_of = jnp.where(present > 0.5, rank, -1.0)[0:1, :].astype(jnp.int32)
        pick = jnp.where(
            lax.broadcasted_iota(jnp.int32, (depth, SAMPLES), 0) == place_of, 1.0, 0.0
        ).astype(bf16)
    often = jnp.where(times > OFTEN + 0.5, float(SAMPLES), 0.0)
    count_out[0] = jnp.sum((present + often)[0:1, :].astype(jnp.int32))
    times = times[0:1, :]
    load_values.wait()
    values = values_in[...]
    mean = jnp.sum(values * times, axis=1, keepdims=True) * (1.0 / SAMPLES)
    centered = values - mean
    total = jnp.sum(centered * centered * times, axis=1, keepdims=True)
    scaled = (centered * lax.rsqrt(total + 1e-06)).astype(bf16)
    if compact:
        weighted = (scaled.astype(f32) * times).astype(bf16)
        side = lax.dot_general(weighted, pick, NT, preferred_element_type=f32)
        front = lax.dot_general(scaled, pick, NT, preferred_element_type=f32)
    else:
        every = jnp.dot(scaled, hits, preferred_element_type=f32)
        side = jnp.concatenate([every, jnp.zeros((OWN, depth - SAMPLES), f32)], axis=1)
        front = side
    load_labels.wait()
    marks = labels_in[...].astype(f32)
    module = lax.broadcasted_iota(jnp.int32, (K, depth), 0).astype(f32) - 150.0
    module = jnp.where(lax.broadcasted_iota(jnp.int32, (K, depth), 1) == depth - 1, module, 0.0)
    front = front + lax.dot_general(
        marks.astype(bf16), module.astype(bf16), (((0,), (0,)), ((), ())),
        preferred_element_type=f32,
    )
    front = front.astype(bf16)
    rows[pl.ds(pl.multiple_of(core * OWN, OWN), OWN), :] = side.astype(bf16)
    cols[0:HALF, :] = front[0:HALF]
    cols[EARLY // 2 : EARLY // 2 + HALF, :] = front[HALF:OWN]
    place_xc = x * 2 + core
    module = lax.broadcasted_iota(jnp.int32, (K, OWN), 0).astype(f32) - 150.0
    info[place_xc, 0:1, :] = jnp.full((1, KEEP), -1000.0, f32)
    info[place_xc, 1:2, :] = jnp.zeros((1, KEEP), f32)
    info[place_xc, 0:1, 0:OWN] = jnp.sum(marks * module, axis=0, keepdims=True)
    info[place_xc, 1:2, 0:OWN] = ref_kim[...]

    pl.semaphore_wait(barrier, len(peers))

    def row_block(chunk, c):
        return rows.at[pl.ds(pl.multiple_of(chunk * CHUNK + c * OWN, OWN), OWN), :]

    def col_block(step, part, slot):
        if step == LINE - 1:
            at = LINE * EARLY + part * (LATE // 2) + slot * HALF
        elif slot == LINE - 1:
            at = (LINE - 1) * EARLY + step * OWN + part * HALF
        else:
            at = step * EARLY + part * (EARLY // 2) + slot * HALF
        return cols.at[pl.ds(at, HALF), :]

    def near_index(part, place):
        return part * LINE + place

    def far_index(part, step, slot):
        return (part * LINE + step) * LINE + slot

    along = (at_z, at_y)
    across = (at_y, at_z)

    def group(place, flip):
        if place == 0:
            return partner
        return at_x(place) if flip == 0 else at_x(place, other)

    mates = [(0, 1)] + [(place, flip) for place in range(1, LINE) for flip in range(2)]

    def to_mates(buffer, send_sem, recv_sem):
        for place, flip in mates:
            send(
                buffer.at[place_xc], buffer.at[place_xc], send_sem.at[place * 2 + flip],
                recv_sem.at[SEEN_AS[place] * 2 + flip], group(place, flip),
            )

    def from_mates(buffer, send_sem, recv_sem):
        for place, flip in mates:
            there = lax.rem(x + OFFSETS[place], LINE) * 2 + (core if flip == 0 else other)
            remote(
                buffer.at[there], buffer.at[there], send_sem.at[place * 2 + flip],
                recv_sem.at[place * 2 + flip], group(place, flip),
            ).wait_recv()

    def far_copy(part, slot, place):
        return remote(
            col_block(0, part, slot), col_block(SEEN_AS[place], part, slot),
            send_far.at[far_index(part, place, slot)],
            recv_far.at[far_index(part, SEEN_AS[place], slot)], across[part](place),
        )

    def forward_columns(part, slot, places):
        for place in places:
            far_copy(part, slot, place).start()

    def send_near_columns(place):
        for part in range(2):
            send(
                col_block(0, part, 0), col_block(0, part, SEEN_AS[place]),
                send_near.at[near_index(part, place)],
                recv_near.at[near_index(part, SEEN_AS[place])], along[part](place),
            )

    def send_rows_to(place):
        send(
            row_block(0, core), row_block(SEEN_AS[place], core),
            send_rows.at[place], recv_rows.at[SEEN_AS[place]], at_x(place),
        )

    def own_rows():
        send(row_block(0, core), row_block(0, core), send_fwd.at[0], recv_fwd.at[0], partner)

    send_near_columns(1)
    send_near_columns(2)
    own_rows()
    to_mates(info, send_info, recv_info)
    def wait_near(part, place):
        block = col_block(0, part, place)
        remote(
            block, block, send_near.at[near_index(part, place)],
            recv_near.at[near_index(part, place)], along[part](place),
        ).wait_recv()

    def wait_far(step, slots):
        for part in range(2):
            for slot in slots:
                block = col_block(step, part, slot)
                remote(
                    block, block, send_far.at[far_index(part, step, slot)],
                    recv_far.at[far_index(part, step, slot)], across[part](step),
                ).wait_recv()

    def pass_rows(chunk):
        block = row_block(chunk, core)
        remote(block, block, send_rows.at[chunk], recv_rows.at[chunk], at_x(chunk)).wait_recv()
        copy = remote(block, block, send_fwd.at[chunk], recv_fwd.at[chunk], partner)
        copy.start()

    def wait_rows(chunk):
        block = row_block(chunk, other)
        remote(block, block, send_fwd.at[chunk], recv_fwd.at[chunk], partner).wait_recv()

    for part in range(2):
        forward_columns(part, 0, (1, 2))
    send_rows_to(1)
    send_rows_to(2)
    send_rows_to(3)

    acc[...] = jnp.zeros_like(acc)
    for place in range(1, LINE - 1):
        for part in range(2):
            wait_near(part, place)
            forward_columns(part, place, (1, 2))
    send_near_columns(LINE - 1)
    for slot in range(LINE - 1):
        for part in range(2):
            forward_columns(part, slot, (LINE - 1,))
    wait_rows(0)

    def take_info():
        from_mates(info, send_info, recv_info)
        which = lax.broadcasted_iota(jnp.int32, (KP, KEEP), 0).astype(f32) - 150.0
        for index in range(2 * LINE):
            side_lt[:, index * KEEP : (index + 1) * KEEP] = jnp.where(
                which == info[index, 0:1, :], 1.0, 0.0
            ).astype(bf16)
        blank = jnp.zeros((1, CHUNK - KEEP), f32)
        for chunk in range(LINE):
            there = lax.rem(x + OFFSETS[chunk], LINE) * 2
            first = jnp.concatenate([info[there, 0:1, :] + 1000.0, blank], axis=1)
            second = jnp.concatenate([info[there + 1, 0:1, :] + 1000.0, blank], axis=1)
            both = first + pltpu.roll(second, OWN, 1) - 1000.0
            side_ids[0:1, chunk * CHUNK : (chunk + 1) * CHUNK] = both

    def pair_slice(chunk, c):
        return acc.at[:, pl.ds(pl.multiple_of(chunk * CHUNK + c * 256, 128), KEEP)]

    def to_partner(chunk):
        return remote(
            pair_slice(chunk, other), pair.at[chunk], send_pair.at[chunk], recv_pair.at[chunk],
            partner,
        )

    ours = (lax.broadcasted_iota(jnp.int32, (KP // 2, 128), 1) < 64) == (core == 0)

    def summed(chunk):
        whole_at = pl.multiple_of(chunk * CHUNK + core * 384, 128)
        main = acc[:, pl.ds(whole_at, 256)]
        main = main + pair[chunk, :, pl.ds(pl.multiple_of(core * 128, 128), 256)]
        shared = acc[:, chunk * CHUNK + 256 : chunk * CHUNK + 384]
        shared = shared + pair[chunk, :, pl.ds(pl.multiple_of((1 - core) * 256, 128), 128)]
        return main, shared

    def to_owner(chunk):
        return [
            remote(
                src.at[chunk], dst.at[SEEN_AS[chunk]], send_sum.at[first + chunk],
                recv_sum.at[first + SEEN_AS[chunk]], at_x(chunk),
            )
            for src, dst, first in ((sent, got, 0), (sent_shared, got_shared, LINE))
        ]

    def pass_sum(chunk):
        to_partner(chunk).wait_recv()
        main, shared = summed(chunk)
        sent[chunk] = main.astype(bf16)
        upper = pltpu.roll(shared[KP // 2 : KP], 64, 1)
        sent_shared[chunk] = jnp.where(ours, shared[0 : KP // 2], upper).astype(bf16)
        for copy in to_owner(chunk):
            copy.start()

    def make_labels(base, width):
        last = lax.broadcasted_iota(jnp.int32, (16, depth), 1) == depth - 1
        ids = lax.dot_general(
            jnp.where(last, 1.0, 0.0).astype(bf16), cols[pl.ds(base, width), :], NT,
            preferred_element_type=f32,
        )
        which = lax.broadcasted_iota(jnp.int32, (KP, width), 0).astype(f32) - 150.0
        return jnp.where(which == ids[0:1, :], 1.0, 0.0).astype(bf16)

    def score(into, base, width, side_at):
        side_block = rows[pl.ds(side_at, TILE), :]
        for start in range(0, width, 256):
            size = min(256, width - start)
            scores = lax.dot_general(
                cols[pl.ds(base + start, size), :], side_block, NT, preferred_element_type=f32
            )
            squares = scores * scores
            into[start : start + size, :] = (squares * squares * squares).astype(bf16)

    def count(held, width, side_at, module_rows):
        acc[:, pl.ds(side_at, TILE)] += jnp.dot(
            module_rows, held[0:width, :], preferred_element_type=f32
        )

    soon = (LINE - 1) * 3
    later = soon + (LINE - 1) * 2

    def task(t):
        group = jnp.where(
            t < soon, t // 3, jnp.where(t < later, (t - soon) // 2, LINE - 1)
        )
        tile = jnp.where(
            t < soon, lax.rem(t, 3), jnp.where(t < later, 3 + lax.rem(t + 1, 2), t - later)
        )
        return group, pl.multiple_of(group * EARLY, HALF), pl.multiple_of(tile * TILE, TILE)

    def score_task(into, t):
        group, base, side_at = task(t)
        score(into, base, EARLY, side_at)

    def count_task(held, t):
        group, base, side_at = task(t)
        count(held, EARLY, side_at, lt[group])

    lt[0] = make_labels(0, EARLY)
    score_task(even, 0)
    pass_rows(1)
    pass_rows(2)
    take_info()

    def two_tiles(u, carry):
        @pl.when(u == 0)
        def _():
            wait_rows(1)
            wait_rows(2)

        for far in range(1, LINE - 1):

            @pl.when(u == far)
            def _():
                wait_far(far, range(LINE - 1))
                lt[far] = make_labels(far * EARLY, EARLY)
                if far == LINE - 2:
                    for part in range(2):
                        wait_near(part, LINE - 1)
                        forward_columns(part, LINE - 1, (1, 2, 3))
                    pass_rows(3)

        @pl.when(u == (soon - 1) // 2)
        def _():
            wait_rows(3)

        @pl.when(u == (later - 1) // 2)
        def _():
            wait_far(1, (LINE - 1,))
            wait_far(2, (LINE - 1,))
            lt[LINE - 1] = make_labels((LINE - 1) * EARLY, EARLY)

        count_task(even, 2 * u)
        score_task(odd, 2 * u + 1)
        count_task(odd, 2 * u + 1)
        score_task(even, 2 * u + 2)
        return carry

    pairs = (later + TILES - 2) // 2
    lax.fori_loop(0, pairs, two_tiles, 0)
    count_task(even, 2 * pairs)
    score_task(odd, 2 * pairs + 1)
    wait_far(LINE - 1, range(LINE))
    lt_late[...] = make_labels(LINE * EARLY, LATE)
    count_task(odd, 2 * pairs + 1)
    score(even, LINE * EARLY, LATE, (TILES - 1) * TILE)
    for turn in range(TILES):
        side_at = (TILES - 1 - turn) * TILE
        held, into = (even, odd) if turn % 2 == 0 else (odd, even)
        count(held, LATE, side_at, lt_late[...])
        if turn < TILES - 1:
            score(into, LINE * EARLY, LATE, side_at - TILE)
        which = lax.broadcasted_iota(jnp.int32, (KP, TILE), 0).astype(f32) - 150.0
        done = acc[:, side_at : side_at + TILE]
        hit = which == side_ids[0:1, side_at : side_at + TILE]
        kim_rows[0:1, side_at : side_at + TILE] = jnp.sum(
            jnp.where(hit, done, 0.0), axis=0, keepdims=True
        )
        kim_rows[1:2, side_at : side_at + TILE] = jnp.sum(done, axis=0, keepdims=True)
        if turn > 0:
            to_partner(LINE - turn).start()

    for chunk in range(LINE):
        there = lax.rem(x + OFFSETS[chunk], LINE) * 2
        for c in range(2):
            for kind in range(2):
                piece = kim_rows[kind : kind + 1, chunk * CHUNK + c * 256 : chunk * CHUNK + c * 256 + KEEP]
                if c == 1:
                    piece = pltpu.roll(piece, KEEP - 64, 1)
                parts[place_xc, kind, pl.ds(there + c, 1), :] = piece
    to_mates(parts, send_part, recv_part)
    for chunk in range(LINE - 1, 0, -1):
        pass_sum(chunk)

    from_mates(parts, send_part, recv_part)
    kim, rowsum = parts[0, 0], parts[0, 1]
    for index in range(1, 2 * LINE):
        kim = kim + parts[index, 0]
        rowsum = rowsum + parts[index, 1]
    for index in range(2 * LINE):
        at = slice(index * KEEP, (index + 1) * KEEP)
        k, r, ref = kim[index : index + 1], rowsum[index : index + 1], info[index, 1:2, :]
        one, none = jnp.ones_like(k), jnp.zeros_like(k)
        stats[:, at] = jnp.concatenate([k, k * k, ref, ref * ref, k * ref, r, one, none], axis=0)
    exact = stats[...]
    high = exact.astype(bf16).astype(f32)
    middle = (exact - high).astype(bf16).astype(f32)
    low = exact - high - middle
    split = jnp.concatenate([high, middle, low, jnp.zeros_like(low)], axis=0).astype(bf16)
    sums = lax.dot_general(split, side_lt[...], NT, preferred_element_type=f32)
    total_sums = sums[0:8] + sums[8:16] + sums[16:24]

    def wait_sent(copies):
        for copy in copies:
            copy.wait_send()

    for axis, (mine, buffer, at) in enumerate(((y, sums_y, at_y), (z, sums_z, at_z))):
        buffer[mine] = total_sums
        copies = []
        for place in range(1, LINE):
            copy = remote(
                buffer.at[mine], buffer.at[mine], send_yz.at[axis * LINE + place],
                recv_yz.at[axis * LINE + SEEN_AS[place]], at(place),
            )
            copy.start()
            copies.append(copy)
        for place in range(1, LINE):
            there = lax.rem(mine + OFFSETS[place], LINE)
            remote(
                buffer.at[there], buffer.at[there], send_yz.at[axis * LINE + place],
                recv_yz.at[axis * LINE + place], at(place),
            ).wait_recv()
        total_sums = buffer[0]
        for index in range(1, LINE):
            total_sums = total_sums + buffer[index]
        wait_sent(copies)

    s_k, s_kk, s_y, s_yy, s_ky, s_r, n = (total_sums[i : i + 1, 0:K] for i in range(7))
    mean_x = s_k / (n * n)
    var_x = jnp.maximum(s_kk / (n * n * n) - mean_x * mean_x, 0.0001)
    mean_y = s_y / n
    var_y = jnp.maximum(s_yy / n - mean_y * mean_y, 0.01)
    cross = s_ky / (n * n) - mean_x * mean_y
    between = (s_r - s_k) / (n * (float(G) - n))
    pres_out[0:1, :] = (mean_x - between) * jnp.sqrt(n / var_x)
    pres_out[1:2, :] = cross * jnp.sqrt(n / (var_x * var_y))

    to_partner(0).wait_recv()
    main, shared = summed(0)
    for chunk in range(1, LINE):
        for src, dst, first in ((sent, got, 0), (sent_shared, got_shared, LINE)):
            remote(
                src.at[chunk], dst.at[chunk], send_sum.at[first + chunk],
                recv_sum.at[first + chunk], at_x(chunk),
            ).wait_recv()
        main = main + got[chunk].astype(f32)
        lower = got_shared[chunk].astype(f32)
        shared = shared + jnp.concatenate([lower, pltpu.roll(lower, 64, 1)], axis=0)
    conn = jnp.where(
        core == 0,
        jnp.concatenate([main, shared], axis=1),
        pltpu.roll(jnp.concatenate([shared, main], axis=1), KEEP - 64, 1),
    )
    conn_out[...] = conn[0:K, 0:OWN]

    wait_sent(started)
    for place in range(1, LINE):
        for part in range(2):
            for slot in range(LINE):
                far_copy(part, slot, place).wait_send()
    for chunk in range(1, LINE):
        block = row_block(chunk, core)
        remote(block, block, send_fwd.at[chunk], recv_fwd.at[chunk], partner).wait_send()
        for copy in to_owner(chunk):
            copy.wait_send()
    for chunk in range(LINE):
        to_partner(chunk).wait_send()


def whole(depth, compact, collective, resample, expression, labels, ref_kim):
    f32, bf16 = jnp.float32, jnp.bfloat16
    dma = pltpu.SemaphoreType.DMA
    vmem, hbm = pl.BlockSpec(memory_space=pltpu.VMEM), pl.BlockSpec(memory_space=pl.ANY)
    scratch = [
        pltpu.VMEM((OWN, SAMPLES), f32),
        pltpu.VMEM((K, OWN), jnp.int32),
        pltpu.VMEM((ROWS, depth), bf16),
        pltpu.VMEM((COLS, depth), bf16),
        pltpu.VMEM((LINE, KP, EARLY), bf16),
        pltpu.VMEM((KP, LATE), bf16),
        pltpu.VMEM((LATE, TILE), bf16),
        pltpu.VMEM((LATE, TILE), bf16),
        pltpu.VMEM((KP, ROWS), f32),
        pltpu.VMEM((LINE, KP, KEEP), f32),
        pltpu.VMEM((LINE, KP, 256), bf16),
        pltpu.VMEM((LINE, KP, 256), bf16),
        pltpu.VMEM((LINE, KP // 2, 128), bf16),
        pltpu.VMEM((LINE, KP // 2, 128), bf16),
        pltpu.VMEM((2 * LINE, 2, KEEP), f32),
        pltpu.VMEM((8, ROWS), f32),
        pltpu.VMEM((KP, 2 * LINE * KEEP), bf16),
        pltpu.VMEM((8, ROWS), f32),
        pltpu.VMEM((2 * LINE, 2, 2 * LINE, KEEP), f32),
        pltpu.VMEM((8, 2 * LINE * KEEP), f32),
        pltpu.VMEM((LINE, 8, KP), f32),
        pltpu.VMEM((LINE, 8, KP), f32),
        dma((2,)),
    ]
    for count in (
        LINE, LINE, 2 * LINE, 2 * LINE * LINE, LINE, 2 * LINE, 2 * LINE, 2 * LINE, 2 * LINE,
    ):
        scratch += [dma((count,)), dma((count,))]
    return pl.pallas_call(
        functools.partial(kernel, depth, compact),
        out_shape=(
            jax.ShapeDtypeStruct((K, OWN), f32),
            jax.ShapeDtypeStruct((2, K), f32),
            jax.ShapeDtypeStruct((1,), jnp.int32),
        ),
        in_specs=[vmem, hbm, hbm, vmem],
        out_specs=(vmem, vmem, pl.BlockSpec(memory_space=pltpu.SMEM)),
        scratch_shapes=scratch,
        compiler_params=pltpu.CompilerParams(
            collective_id=collective, has_side_effects=True, vmem_limit_bytes=60 * 1024 * 1024
        ),
        name=f"network_{depth}",
    )(resample, expression, labels, ref_kim)


def local(expression, resample, labels, ref_kim):
    operands = (
        resample.reshape(1, SAMPLES), expression.T, labels.T, ref_kim.reshape(1, OWN),
    )
    conn, preservation, distinct = whole(256, True, 0, *operands)
    conn, preservation = lax.cond(
        distinct[0] <= 255,
        lambda *ready: ready[:2],
        lambda *ready: whole(512, False, 1, *ready[2:])[:2],
        conn, preservation, *operands,
    )
    return conn.T, preservation


def solution(mesh):
    torus = Mesh(mesh.devices.reshape(4, 4, 2, 2, 2), AXES)
    placed = (P(None, AXES), P(), P(AXES, None), P(AXES))
    return jax.shard_map(
        local, mesh=torus, in_specs=placed, out_specs=(P(AXES, None), P()), check_vma=False
    )
```
